32 devices in a mesh: lat: 4 (over y, x), lon: 8 (over z, core).
Axes of the slice: x: 2, y: 2, z: 4, core: 2. Of those that a mesh axis runs over, the one named last changes fastest.
Arguments:
- input_field: bfloat16 [512, 512, 128], P('lat', 'lon'), may hold values from -6 to 6
- conv_one: bfloat16 [3, 3, 128, 128], replicated, may hold values from -0.1875 to 0.1875
- conv_two: bfloat16 [3, 3, 128, 128], replicated, may hold values from -0.1875 to 0.1875
- merge_weight: bfloat16 [512, 512], replicated, may hold values from -0.25 to 0.25
- norm_gains: float32 [4, 512], replicated, may hold values from 0.1 to 1.9
- attention_in: bfloat16 [512, 1536], replicated, may hold values from -0.25 to 0.25
- attention_out: bfloat16 [512, 512], replicated, may hold values from -0.25 to 0.25
- dense_in: bfloat16 [512, 2048], replicated, may hold values from -0.25 to 0.25
- dense_out: bfloat16 [2048, 512], replicated, may hold values from -0.125 to 0.125
- expand_weight: bfloat16 [512, 512], replicated, may hold values from -0.25 to 0.25
Outputs:
- output_field: bfloat16 [512, 512, 128], P('lat', 'lon')
The draws below stay inside these ranges and needn't reach their ends.
All inputs are finite; a program needn't handle non-finite values.
Results may differ from the reference program's by a relative error of at most 0.0095.
Values may be sent and summed in bfloat16 or wider, within the bound.
A program may use at most 128 MiB of HBM per device.

```python
import jax
import jax.numpy as jnp
from jax import lax

CHANNELS = 128
LATENT = 512
NUM_HEADS = 16
MLP_WIDTH = 2048
WINDOW = 16
HEAD_WIDTH = 32
LAT_CELLS = 512
LON_CELLS = 512


def level_of(stream_key, dims, shards, smallest, largest):
    factor_of = 1.0
    for axis_at, blocks in shards:
        draws = jax.random.uniform(jax.random.fold_in(jax.random.fold_in(stream_key, 6), axis_at), (blocks,), jnp.float32, smallest / len(shards), largest / len(shards))
        factor_of = factor_of * jnp.repeat(jnp.exp(draws), dims[axis_at] // blocks).reshape((-1,) + (1,) * (len(dims) - 1 - axis_at))
    return factor_of


def gaussian(own_key, extent, scale, bound, shards=(), kind=jnp.bfloat16):
    entries = scale * jax.random.normal(own_key, extent, jnp.float32)
    if shards:
        entries = entries * level_of(own_key, extent, shards, -0.22, 0.18)
    return jnp.clip(entries, -bound, bound).astype(kind)


def setup_inputs(seed: int = 0) -> dict:
    keys = jax.random.split(jax.random.key(seed), 11)
    return {
        "input_field": gaussian(keys[0], (LAT_CELLS, LON_CELLS, CHANNELS), 1.0, 6.0, ((0, 4), (1, 8))),
        "conv_one": gaussian(keys[1], (3, 3, CHANNELS, CHANNELS), (9 * CHANNELS) ** -0.5, 0.1875),
        "conv_two": gaussian(keys[2], (3, 3, CHANNELS, CHANNELS), (9 * CHANNELS) ** -0.5, 0.1875),
        "merge_weight": gaussian(keys[3], (4 * CHANNELS, LATENT), (4 * CHANNELS) ** -0.5, 0.25),
        "norm_gains": jnp.clip(1.0 + 0.18 * jax.random.normal(keys[4], (4, LATENT), jnp.float32), 0.1, 1.9),
        "attention_in": gaussian(keys[5], (LATENT, 3 * LATENT), LATENT ** -0.5, 0.25),
        "attention_out": gaussian(keys[6], (LATENT, LATENT), LATENT ** -0.5, 0.25),
        "dense_in": gaussian(keys[7], (LATENT, MLP_WIDTH), LATENT ** -0.5, 0.25),
        "dense_out": gaussian(keys[8], (MLP_WIDTH, LATENT), MLP_WIDTH ** -0.5, 0.125),
        "expand_weight": gaussian(keys[9], (LATENT, 4 * CHANNELS), LATENT ** -0.5, 0.25),
    }


EPSILON = 1e-06
FLOOR = 0.75

def conv_gelu(source, kernel, padding):
    result = lax.conv_general_dilated(source[None], kernel, (1, 1), padding, dimension_numbers=('NHWC', 'HWIO', 'NHWC'), preferred_element_type=jnp.float32)[0]
    return jax.nn.gelu(result)

def layer_norm(stream, gain):
    center = stream - lax.optimization_barrier(jnp.mean(stream, axis=-1, keepdims=True))
    spread = lax.optimization_barrier(jnp.mean(center * center, axis=-1, keepdims=True))
    return center * lax.rsqrt(spread + EPSILON) * gain

def head_norm(stream, gain):
    square = lax.optimization_barrier(jnp.mean(stream * stream, axis=-1, keepdims=True))
    return stream * gain / jnp.sqrt(jnp.maximum(square, FLOOR))

def project_heads(tokens, norm_gains, attention_in):
    count = tokens.shape[0]
    normed = layer_norm(tokens.astype(jnp.float32), norm_gains[0]).astype(jnp.bfloat16)
    projected = jnp.dot(normed, attention_in, preferred_element_type=jnp.float32)
    split_shape = (count, NUM_HEADS, HEAD_WIDTH)
    queries = head_norm(projected[:, :LATENT].reshape(split_shape), norm_gains[1].reshape(NUM_HEADS, HEAD_WIDTH)).astype(jnp.bfloat16)
    key_rows = head_norm(projected[:, LATENT:2 * LATENT].reshape(split_shape), norm_gains[2].reshape(NUM_HEADS, HEAD_WIDTH)).astype(jnp.bfloat16)
    values = projected[:, 2 * LATENT:].reshape(split_shape).astype(jnp.bfloat16)
    return (queries, key_rows, values)

def attend_window(queries, key_rows, values):
    scores = jnp.einsum('qhd,khd->hqk', queries.astype(jnp.float32), key_rows.astype(jnp.float32)) * HEAD_WIDTH ** (-0.5)
    expon = jnp.exp(scores)
    weights = (expon / lax.optimization_barrier(jnp.sum(expon, axis=-1, keepdims=True))).astype(jnp.bfloat16)
    gathered = jnp.einsum('hqk,khd->qhd', weights.astype(jnp.float32), values.astype(jnp.float32))
    return gathered.reshape(queries.shape[0], LATENT).astype(jnp.bfloat16)

def finish(tokens, attended, norm_gains, attention_out, dense_in, dense_out):
    mixed_tokens = (tokens.astype(jnp.float32) + jnp.dot(attended, attention_out, preferred_element_type=jnp.float32)).astype(jnp.bfloat16)
    normed_two = layer_norm(mixed_tokens.astype(jnp.float32), norm_gains[3]).astype(jnp.bfloat16)
    inner_units = jax.nn.gelu(jnp.dot(normed_two, dense_in, preferred_element_type=jnp.float32)).astype(jnp.bfloat16)
    return (mixed_tokens.astype(jnp.float32) + jnp.dot(inner_units, dense_out, preferred_element_type=jnp.float32)).astype(jnp.bfloat16)

def reference(input_field, conv_one, conv_two, merge_weight, norm_gains, attention_in, attention_out, dense_in, dense_out, expand_weight):
    first = conv_gelu(input_field, conv_one, 'SAME').astype(jnp.bfloat16)
    second = conv_gelu(first, conv_two, 'SAME').astype(jnp.bfloat16)
    half_lat = LAT_CELLS // 2
    half_lon = LON_CELLS // 2
    offset_lat = half_lat // WINDOW
    offset_lon = half_lon // WINDOW
    patches = second.reshape(half_lat, 2, half_lon, 2, CHANNELS).transpose(0, 2, 1, 3, 4).reshape(half_lat * half_lon, 4 * CHANNELS)
    coarse = jnp.dot(patches, merge_weight, preferred_element_type=jnp.float32).astype(jnp.bfloat16)
    grouped = coarse.reshape(WINDOW, offset_lat, WINDOW, offset_lon, LATENT).transpose(1, 3, 0, 2, 4).reshape(offset_lat * offset_lon, WINDOW * WINDOW, LATENT)

    def one_window(tokens):
        queries, key_rows, values = project_heads(tokens, norm_gains, attention_in)
        attended = attend_window(queries, key_rows, values)
        return finish(tokens, attended, norm_gains, attention_out, dense_in, dense_out)
    updated = lax.map(one_window, grouped)
    placed = updated.reshape(offset_lat, offset_lon, WINDOW, WINDOW, LATENT).transpose(2, 0, 3, 1, 4).reshape(half_lat * half_lon, LATENT)
    expanded = jnp.dot(placed, expand_weight, preferred_element_type=jnp.float32)
    expanded = expanded.reshape(half_lat, half_lon, 2, 2, CHANNELS).transpose(0, 2, 1, 3, 4).reshape(LAT_CELLS, LON_CELLS, CHANNELS)
    return (expanded + input_field.astype(jnp.float32)).astype(jnp.bfloat16)
```

```python
import functools
import math

import jax
import jax.numpy as jnp
from jax import lax
from jax.experimental import pallas as pl
from jax.experimental.pallas import tpu as pltpu
from jax.sharding import PartitionSpec as P

WINDOW = 16
HEAD_WIDTH = 32
EPSILON = 1e-06
FLOOR = 0.75
F32 = jnp.float32
BF16 = jnp.bfloat16
LIMIT = 60 * 1024 * 1024
MESH = pl.DeviceIdType.MESH
LEAD = 8
UNIT = 2


def dot(a, b):
    return jnp.dot(a, b, preferred_element_type=F32)


def ones_where(flag):
    return flag.astype(F32).astype(BF16)


def pair_kernel(kernel_ref, paired):
    taps, _, c, o = kernel_ref.shape
    zero = jnp.zeros((c, o), BF16)
    for a in range(taps):
        for b in range(4):
            rows = slice((4 * a + b) * c, (4 * a + b + 1) * c)
            paired[rows, :o] = kernel_ref[a, b] if b < 3 else zero
            paired[rows, o:] = kernel_ref[a, b - 1] if b > 0 else zero


def layer_norm(stream, gain):
    center = stream - jnp.mean(stream, axis=-1, keepdims=True)
    spread = jnp.mean(center * center, axis=-1, keepdims=True)
    return center * lax.rsqrt(spread + EPSILON) * gain


def window_block(windows, sources, tokens, cells, g_ref, ai_ref, ao_ref, di_ref, do_ref):
    latent = cells.shape[-1]
    size = sources * tokens
    count = windows * size
    coarse = cells
    if windows > 1:
        to = lax.broadcasted_iota(jnp.int32, (count, count), 0)
        of = lax.broadcasted_iota(jnp.int32, (count, count), 1)
        row = lax.broadcasted_iota(jnp.int32, (count, 1), 0)
        col = lax.broadcasted_iota(jnp.int32, (1, count), 1)

        def sorted_row(i):
            return (i // tokens % windows) * size + i // (tokens * windows) * tokens + i % tokens

        gather = ones_where(to == sorted_row(col))
        scatter = ones_where(of == sorted_row(row))
        coarse = dot(gather, cells.astype(BF16))
    gains = g_ref[...]
    normed = layer_norm(coarse, gains[0:1]).astype(BF16)
    head_row = lax.broadcasted_iota(jnp.int32, (latent, latent), 0) // HEAD_WIDTH
    head_col = lax.broadcasted_iota(jnp.int32, (latent, latent), 1) // HEAD_WIDTH
    spread = jnp.where(head_row == head_col, 1.0 / HEAD_WIDTH, 0.0).astype(BF16)

    def head_norm(stream, gain):
        square = dot((stream * stream).astype(BF16), spread)
        return (stream * gain * lax.rsqrt(jnp.maximum(square, FLOOR))).astype(BF16)

    queries = head_norm(dot(normed, ai_ref[:, :latent]), gains[1:2])
    key_rows = head_norm(dot(normed, ai_ref[:, latent : 2 * latent]), gains[2:3])
    values = dot(normed, ai_ref[:, 2 * latent :]).astype(BF16)
    group = 128
    heads = group // HEAD_WIDTH
    lane = lax.broadcasted_iota(jnp.int32, (size, group), 1) // HEAD_WIDTH
    marks = [ones_where(lane == h) for h in range(heads)]
    scale = HEAD_WIDTH ** (-0.5) * math.log2(math.e)
    parts = []
    for win in range(windows):
        span = slice(win * size, (win + 1) * size)
        row_parts = []
        for at in range(0, latent, group):
            q = queries[span, at : at + group]
            k = key_rows[span, at : at + group]
            v = values[span, at : at + group]
            expons = []
            stacked = []
            for h in range(heads):
                scores = lax.dot_general(
                    q * marks[h], k, (((1,), (1,)), ((), ())), preferred_element_type=F32
                )
                expons.append(jnp.exp2(scores * scale).astype(BF16))
                stacked.append(jnp.concatenate([v * marks[h], marks[h]], axis=1))
            both = dot(jnp.concatenate(expons, axis=1), jnp.concatenate(stacked, axis=0))
            row_parts.append((both[:, :group] / both[:, group:]).astype(BF16))
        parts.append(jnp.concatenate(row_parts, axis=1))
    attended = jnp.concatenate(parts, axis=0)
    mixed = (coarse + dot(attended, ao_ref[...])).astype(BF16)
    normed_two = layer_norm(mixed.astype(F32), gains[3:4]).astype(BF16)
    total = mixed.astype(F32)
    width = di_ref.shape[1]
    step = min(512, width)
    for at in range(0, width, step):
        inner = jax.nn.gelu(dot(normed_two, di_ref[:, at : at + step])).astype(BF16)
        total = total + dot(inner, do_ref[at : at + step, :])
    if windows > 1:
        total = dot(scatter, total.astype(BF16))
    return total


def whole_body(geo, x_hbm, k1_hbm, k2_hbm, mw_hbm, g_hbm, ai_hbm, ao_hbm, di_hbm, do_hbm, ew_hbm, out_hbm,
               xv, k1_ref, k2_ref, mw_ref, g_ref, ai_ref, ao_ref, di_ref, do_ref, ew_ref,
               w1_ref, w2_ref, xs, xn, xf, fs, fn, ff, edges, sides, caps, corners,
               sbuf, rbuf, s2buf, r2buf, os, ost,
               load_sem, halo_send, halo_recv, go_send, go_recv, back_send, back_recv, out_sem):
    (nlat, nlon, bands, per_lon, offset_lat, offset_lon, pairs, joint, groups) = geo
    count = nlat * nlon
    lat = lax.axis_index("lat")
    lon = lax.axis_index("lon")
    me = lat * nlon + lon
    height, breadth, c = xv.shape
    half = breadth // 2
    latent = 4 * c
    tokens = bands * per_lon
    cells = bands * half
    reach = 2 * offset_lat
    rows = 2 * UNIT
    steps = offset_lat // UNIT
    block = UNIT * offset_lon // joint
    pitch = xs.shape[0] // (height + 4)

    barrier = pltpu.get_barrier_semaphore()

    def greet(k, carry):
        peer = (me + k) % count
        pl.semaphore_signal(barrier, inc=1, device_id=(peer // nlon, peer % nlon), device_id_type=MESH)
        return carry

    lax.fori_loop(1, count, greet, 0)

    loads = [
        pltpu.make_async_copy(a, b, load_sem.at[i])
        for i, (a, b) in enumerate(
            [(x_hbm, xv), (k1_hbm, k1_ref), (k2_hbm, k2_ref), (mw_hbm, mw_ref), (g_hbm, g_ref),
             (ai_hbm, ai_ref), (ao_hbm, ao_ref), (di_hbm, di_ref), (do_hbm, do_ref), (ew_hbm, ew_ref)]
        )
    ]
    for load in loads:
        load.start()
    loads[0].wait()

    def widen(r, carry):
        for k in range(4):
            at = 4 * r + k
            xs[pl.ds((at + 2) * pitch + LEAD, breadth), :] = xv[at].astype(F32)
        return carry

    lax.fori_loop(0, height // 4, widen, 0)

    def column(at):
        return xs[pl.ds(2 * pitch + LEAD + at, height, stride=pitch), :]

    for side, at in enumerate((0, breadth - 2)):
        edges[side] = jnp.concatenate([column(at), column(at + 1)], axis=1).astype(BF16)

    pl.semaphore_wait(barrier, count - 1)

    tip = 16
    ends = (slice(0, tip), slice(height - tip, height))
    halo = []
    for i, (dy, dx) in enumerate(((-1, 0), (1, 0), (0, -1), (0, 1), (-1, -1), (-1, 1), (1, -1), (1, 1))):
        if dx == 0:
            src = xv.at[pl.ds(0 if dy < 0 else height - 2, 2)]
            dst = caps.at[1 if dy < 0 else 0]
        elif dy == 0:
            src = edges.at[0 if dx < 0 else 1]
            dst = sides.at[1 if dx < 0 else 0]
        else:
            first = 0 if dy < 0 else height - tip
            src = edges.at[0 if dx < 0 else 1, pl.ds(first, tip)]
            dst = corners.at[(2 if dy < 0 else 0) + (1 if dx < 0 else 0)]
        there = (lat + dy >= 0) & (lat + dy < nlat) & (lon + dx >= 0) & (lon + dx < nlon)
        back = (lat - dy >= 0) & (lat - dy < nlat) & (lon - dx >= 0) & (lon - dx < nlon)
        copy = pltpu.make_async_remote_copy(
            src_ref=src, dst_ref=dst, send_sem=halo_send.at[i], recv_sem=halo_recv.at[i],
            device_id=(jnp.clip(lat + dy, 0, nlat - 1), jnp.clip(lon + dx, 0, nlon - 1)), device_id_type=MESH,
        )
        halo.append((dy, dx, there, back, copy))
        pl.when(there)(copy.start)

    loads[1].wait()
    pair_kernel(k1_ref, w1_ref)
    loads[2].wait()
    pair_kernel(k2_ref, w2_ref)
    loads[3].wait()

    left, right = LEAD - 2, LEAD + breadth
    for dy, dx, there, back, copy in halo:
        row = 0 if dy > 0 else height + 2
        col = left if dx > 0 else right

        def landed(dy=dy, dx=dx, copy=copy, row=row, col=col):
            copy.wait_recv()
            if dx == 0:
                for k in range(2):
                    xs[pl.ds((row + k) * pitch + LEAD, breadth), :] = caps[0 if dy > 0 else 1, k].astype(F32)
            elif dy == 0:
                value = sides[0 if dx > 0 else 1].astype(F32)
                for k in range(2):
                    xs[pl.ds(2 * pitch + col + k, height, stride=pitch), :] = value[:, k * c : (k + 1) * c]
            else:
                value = corners[(0 if dy > 0 else 2) + (0 if dx > 0 else 1)].astype(F32)
                base = tip - 2 if dy > 0 else 0
                for r in range(2):
                    for k in range(2):
                        xs[pl.ds((row + r) * pitch + col + k, 1), :] = value[
                            base + r : base + r + 1, k * c : (k + 1) * c
                        ]

        def empty(dy=dy, dx=dx, row=row, col=col):
            if dx == 0:
                for k in range(2):
                    xs[pl.ds((row + k) * pitch + LEAD, breadth), :] = jnp.zeros((breadth, c), F32)
            elif dy == 0:
                for k in range(2):
                    xs[pl.ds(2 * pitch + col + k, height, stride=pitch), :] = jnp.zeros((height, c), F32)
            else:
                for r in range(2):
                    for k in range(2):
                        xs[pl.ds((row + r) * pitch + col + k, 1), :] = jnp.zeros((1, c), F32)

        pl.when(back)(landed)
        pl.when(jnp.logical_not(back))(empty)

    def fill(start, n):
        for r in range(n):
            base = (start + r) * pitch + left
            quad = [xs[pl.ds(base + j, pairs, stride=2), :] for j in range(4)]
            xn[pl.ds(start + r, 1)] = jnp.concatenate(quad[:2], axis=1).astype(BF16)[None]
            xf[pl.ds(start + r, 1)] = jnp.concatenate(quad[2:], axis=1).astype(BF16)[None]

    pair = lax.broadcasted_iota(jnp.int32, (pairs, 2 * c), 0)
    lane = lax.broadcasted_iota(jnp.int32, (pairs, 2 * c), 1)
    lon_place = 2 * pair + (lane >= c).astype(jnp.int32) + (lon * breadth - 1)
    inside = (lon_place >= 0) & (lon_place < nlon * breadth)

    def conv_one(starts, n):
        lhs = jnp.concatenate(
            [
                jnp.concatenate(
                    [buf[pl.ds(start + a, n)].reshape(n * pairs, 2 * c) for start in starts], axis=0
                )
                for a in range(3)
                for buf in (xn, xf)
            ],
            axis=1,
        )
        first = jax.nn.gelu(dot(lhs, w1_ref[...])).reshape(bands * n, pairs, 2 * c)
        fs[: bands * n] = jnp.where(inside[None], first, 0.0)
        for p, start in enumerate(starts):
            fn[pl.ds(start, n)] = fs[p * n : (p + 1) * n, 0:half, :].astype(BF16)
            ff[pl.ds(start, n)] = fs[p * n : (p + 1) * n, pl.ds(1, half), :].astype(BF16)

    nothing = jnp.zeros((1, half, 2 * c), BF16)
    for p in range(bands):
        fill(p * reach, 4)
    conv_one([p * reach for p in range(bands)], 2)

    @pl.when(lat == 0)
    def _():
        fn[0:1] = nothing
        ff[0:1] = nothing

    to = lax.broadcasted_iota(jnp.int32, (cells, cells), 0)
    of = lax.broadcasted_iota(jnp.int32, (cells, cells), 1)
    outward = ones_where(of == (to % tokens) * offset_lon + to // tokens)
    inward = ones_where(of == (to % offset_lon) * tokens + to // offset_lon)

    def forward(entry):
        peer = entry % count
        return pltpu.make_async_remote_copy(
            src_ref=sbuf.at[pl.ds(entry, 1)], dst_ref=rbuf.at[pl.ds(entry // count * count + me, 1)],
            send_sem=go_send.at[entry // count], recv_sem=go_recv.at[entry // count],
            device_id=(peer // nlon, peer % nlon), device_id_type=MESH,
        )

    def encode(e, carry):
        base = [p * reach + e * rows for p in range(bands)]
        for start in base:
            fill(start + 4, rows)
        conv_one([start + 2 for start in base], rows)

        @pl.when((lat == nlat - 1) & (e == steps - 1))
        def _():
            fn[height + 1 :] = nothing
            ff[height + 1 :] = nothing

        lhs = jnp.concatenate(
            [
                jnp.concatenate(
                    [buf[pl.ds(start + a, rows)].reshape(rows * half, 2 * c) for start in base], axis=0
                )
                for a in range(3)
                for buf in (fn, ff)
            ],
            axis=1,
        )
        second = jax.nn.gelu(dot(lhs, w2_ref[...])).astype(BF16)
        second = second.reshape(bands * UNIT, 2, half, 2 * c)
        patches = jnp.concatenate(
            [second[:, d].reshape(bands * UNIT * half, 2 * c) for d in range(2)], axis=1
        )
        coarse = dot(patches, mw_ref[...]).astype(BF16).reshape(bands, UNIT, half, latent)
        span = offset_lon // joint
        for u in range(UNIT):
            moved = dot(outward, coarse[:, u].reshape(cells, latent))
            sbuf[pl.ds(e * block + u * span, span)] = moved.reshape(span, joint * tokens, latent).astype(BF16)

        def send(k, carry):
            entry = e * block + (me + k) % block

            @pl.when(entry % count != me)
            def _():
                forward(entry).start()

            @pl.when(entry % count == me)
            def _():
                rbuf[pl.ds(entry, 1)] = sbuf[pl.ds(entry, 1)]

            return carry

        lax.fori_loop(1, block + 1, send, 0)
        return carry

    lax.fori_loop(0, steps, encode, 0)

    for load in loads[4:]:
        load.wait()

    def all_of(buffer, landing, send_sem, recv_sem, g):
        return pltpu.make_async_remote_copy(
            src_ref=buffer.at[pl.ds(0, count - 1)], dst_ref=landing.at[pl.ds(0, count - 1)],
            send_sem=send_sem.at[g], recv_sem=recv_sem.at[g],
            device_id=(lat, (lon + 1) % nlon), device_id_type=MESH,
        )

    def attend(g, carry):
        all_of(sbuf, rbuf, go_send, go_recv, g).wait_recv()
        at = pl.ds(g * count, count)
        cells_in = rbuf[at].astype(F32).reshape(count * joint * tokens, latent)
        total = window_block(joint, count, tokens, cells_in, g_ref, ai_ref, ao_ref, di_ref, do_ref)
        s2buf[at] = total.reshape(count, joint * tokens, latent).astype(BF16)

        def send(k, carry):
            peer = (me + k) % count
            pltpu.make_async_remote_copy(
                src_ref=s2buf.at[pl.ds(g * count + peer, 1)], dst_ref=r2buf.at[pl.ds(g * count + me, 1)],
                send_sem=back_send.at[g], recv_sem=back_recv.at[g],
                device_id=(peer // nlon, peer % nlon), device_id_type=MESH,
            ).start()
            return carry

        lax.fori_loop(1, count, send, 0)
        own = pl.ds(g * count + me, 1)
        r2buf[own] = s2buf[own]
        return carry

    lax.fori_loop(0, groups, attend, 0)

    per_group = steps // groups

    def expand(g, carry):
        all_of(s2buf, r2buf, back_send, back_recv, g).wait_recv()
        for k in range(per_group):
            e = g * per_group + k
            span = offset_lon // joint
            placed = []
            for u in range(UNIT):
                got = r2buf[pl.ds(e * block + u * span, span)].astype(F32).reshape(cells, latent)
                placed.append(dot(inward, got.astype(BF16)).astype(BF16))
            made = dot(jnp.concatenate(placed, axis=0), ew_ref[...])
            for u in range(UNIT):
                for p in range(bands):
                    top = u * cells + p * half
                    for d in range(4):
                        line = (p * rows + 2 * u + d // 2) * breadth + d % 2
                        os[pl.ds(line, half, stride=2), :] = made[top : top + half, d * c : (d + 1) * c]
            for p in range(bands):
                place = pl.ds(p * reach + e * rows, rows)
                lines = os[p * rows * breadth : (p + 1) * rows * breadth, :].reshape(rows, breadth, c)
                ost[place] = (lines + xv[place].astype(F32)).astype(BF16)
                pltpu.make_async_copy(ost.at[place], out_hbm.at[place], out_sem).start()
        return carry

    lax.fori_loop(0, groups, expand, 0)

    def settle(g, carry):
        all_of(sbuf, rbuf, go_send, go_recv, g).wait_send()
        all_of(s2buf, r2buf, back_send, back_recv, g).wait_send()
        return carry

    lax.fori_loop(0, groups, settle, 0)
    for _, _, there, _, copy in halo:
        pl.when(there)(copy.wait_send)
    pltpu.make_async_copy(ost, out_hbm, out_sem).wait()


def per_device(
    input_field,
    conv_one,
    conv_two,
    merge_weight,
    norm_gains,
    attention_in,
    attention_out,
    dense_in,
    dense_out,
    expand_weight,
):
    height, breadth, c = input_field.shape
    latent = merge_weight.shape[1]
    nlat = lax.axis_size("lat")
    nlon = lax.axis_size("lon")
    count = nlat * nlon
    bands = WINDOW // nlat
    per_lon = WINDOW // nlon
    offset_lat = height // (2 * bands)
    offset_lon = breadth // (2 * per_lon)
    tokens = bands * per_lon
    joint = max(1, 8 // tokens)
    entries = offset_lat * offset_lon // joint
    groups = entries // count
    half = breadth // 2
    pairs = -(-(half + 1) // 16) * 16
    pitch = -(-(LEAD + 2 * pairs) // 8) * 8
    rows = 2 * UNIT
    args = (
        input_field, conv_one, conv_two, merge_weight, norm_gains,
        attention_in, attention_out, dense_in, dense_out, expand_weight,
    )
    geo = (nlat, nlon, bands, per_lon, offset_lat, offset_lon, pairs, joint, groups)
    message = (entries, joint * tokens, latent)
    scratch = [pltpu.VMEM(a.shape, a.dtype) for a in args]
    scratch += [
        pltpu.VMEM((12 * c, 2 * c), BF16),
        pltpu.VMEM((12 * c, 2 * c), BF16),
        pltpu.VMEM(((height + 4) * pitch, c), F32),
        pltpu.VMEM((height + 4, pairs, 2 * c), BF16),
        pltpu.VMEM((height + 4, pairs, 2 * c), BF16),
        pltpu.VMEM((bands * rows, pairs, 2 * c), F32),
        pltpu.VMEM((height + 2, half, 2 * c), BF16),
        pltpu.VMEM((height + 2, half, 2 * c), BF16),
        pltpu.VMEM((2, height, 2 * c), BF16),
        pltpu.VMEM((2, height, 2 * c), BF16),
        pltpu.VMEM((2, 2, breadth, c), BF16),
        pltpu.VMEM((4, 16, 2 * c), BF16),
        pltpu.VMEM(message, BF16),
        pltpu.VMEM(message, BF16),
        pltpu.VMEM(message, BF16),
        pltpu.VMEM(message, BF16),
        pltpu.VMEM((bands * rows * breadth, c), F32),
        pltpu.VMEM((height, breadth, c), BF16),
        pltpu.SemaphoreType.DMA((10,)),
        pltpu.SemaphoreType.DMA((8,)),
        pltpu.SemaphoreType.DMA((8,)),
        pltpu.SemaphoreType.DMA((groups,)),
        pltpu.SemaphoreType.DMA((groups,)),
        pltpu.SemaphoreType.DMA((groups,)),
        pltpu.SemaphoreType.DMA((groups,)),
        pltpu.SemaphoreType.DMA,
    ]
    return pl.pallas_call(
        functools.partial(whole_body, geo),
        in_specs=[pl.BlockSpec(memory_space=pl.ANY)] * len(args),
        out_specs=pl.BlockSpec(memory_space=pl.ANY),
        out_shape=jax.ShapeDtypeStruct(input_field.shape, BF16),
        scratch_shapes=scratch,
        compiler_params=pltpu.CompilerParams(
            collective_id=0, has_side_effects=True, vmem_limit_bytes=LIMIT
        ),
        cost_estimate=pl.CostEstimate(flops=40_000_000_000, bytes_accessed=16_000_000, transcendentals=0),
        name="whole",
    )(*args)


def solution(mesh):
    return jax.shard_map(
        per_device,
        mesh=mesh,
        in_specs=(P("lat", "lon", None), P(), P(), P(), P(), P(), P(), P(), P(), P()),
        out_specs=P("lat", "lon", None),
        check_vma=False,
    )
```

```python
import functools
import math

import jax
import jax.numpy as jnp
from jax import lax
from jax.experimental import pallas as pl
from jax.experimental.pallas import tpu as pltpu
from jax.sharding import PartitionSpec as P

WINDOW = 16
HEAD_WIDTH = 32
EPSILON = 1e-06
FLOOR = 0.75
F32 = jnp.float32
BF16 = jnp.bfloat16
LIMIT = 56 * 1024 * 1024
MESH = pl.DeviceIdType.MESH
LEAD = 8
UNIT = 2
EARLY = 2
EARLY_AT = 1


def dot(a, b):
    return jnp.dot(a, b, preferred_element_type=F32)


def ones_where(flag):
    return flag.astype(F32).astype(BF16)


def pair_kernel(kernel_ref, paired):
    taps, _, c, o = kernel_ref.shape
    zero = jnp.zeros((c, o), BF16)
    for a in range(taps):
        for b in range(4):
            rows = slice((4 * a + b) * c, (4 * a + b + 1) * c)
            paired[rows, :o] = kernel_ref[a, b] if b < 3 else zero
            paired[rows, o:] = kernel_ref[a, b - 1] if b > 0 else zero


def layer_norm(stream, gain):
    center = stream - jnp.mean(stream, axis=-1, keepdims=True)
    spread = jnp.mean(center * center, axis=-1, keepdims=True)
    return center * lax.rsqrt(spread + EPSILON) * gain


def window_block(windows, sources, tokens, cells, g_ref, ai_ref, ao_ref, di_ref, do_ref):
    latent = cells.shape[-1]
    size = sources * tokens
    count = windows * size
    coarse = cells
    if windows > 1:
        to = lax.broadcasted_iota(jnp.int32, (count, count), 0)
        of = lax.broadcasted_iota(jnp.int32, (count, count), 1)
        row = lax.broadcasted_iota(jnp.int32, (count, 1), 0)
        col = lax.broadcasted_iota(jnp.int32, (1, count), 1)

        def sorted_row(i):
            return (i // tokens % windows) * size + i // (tokens * windows) * tokens + i % tokens

        gather = ones_where(to == sorted_row(col))
        scatter = ones_where(of == sorted_row(row))
        coarse = dot(gather, cells.astype(BF16))
    gains = g_ref[...]
    normed = layer_norm(coarse, gains[0:1]).astype(BF16)
    head_row = lax.broadcasted_iota(jnp.int32, (latent, latent), 0) // HEAD_WIDTH
    head_col = lax.broadcasted_iota(jnp.int32, (latent, latent), 1) // HEAD_WIDTH
    spread = jnp.where(head_row == head_col, 1.0 / HEAD_WIDTH, 0.0).astype(BF16)

    def head_norm(stream, gain):
        square = dot((stream * stream).astype(BF16), spread)
        return (stream * gain * lax.rsqrt(jnp.maximum(square, FLOOR))).astype(BF16)

    queries = head_norm(dot(normed, ai_ref[:, :latent]), gains[1:2])
    key_rows = head_norm(dot(normed, ai_ref[:, latent : 2 * latent]), gains[2:3])
    values = dot(normed, ai_ref[:, 2 * latent :]).astype(BF16)
    group = 128
    heads = group // HEAD_WIDTH
    lane = lax.broadcasted_iota(jnp.int32, (size, group), 1) // HEAD_WIDTH
    marks = [ones_where(lane == h) for h in range(heads)]
    scale = HEAD_WIDTH ** (-0.5) * math.log2(math.e)
    parts = []
    for win in range(windows):
        span = slice(win * size, (win + 1) * size)
        row_parts = []
        for at in range(0, latent, group):
            q = queries[span, at : at + group]
            k = key_rows[span, at : at + group]
            v = values[span, at : at + group]
            expons = []
            stacked = []
            for h in range(heads):
                scores = lax.dot_general(
                    q * marks[h], k, (((1,), (1,)), ((), ())), preferred_element_type=F32
                )
                expons.append(jnp.exp2(scores * scale).astype(BF16))
                stacked.append(jnp.concatenate([v * marks[h], marks[h]], axis=1))
            both = dot(jnp.concatenate(expons, axis=1), jnp.concatenate(stacked, axis=0))
            row_parts.append((both[:, :group] / both[:, group:]).astype(BF16))
        parts.append(jnp.concatenate(row_parts, axis=1))
    attended = jnp.concatenate(parts, axis=0)
    mixed = (coarse + dot(attended, ao_ref[...])).astype(BF16)
    normed_two = layer_norm(mixed.astype(F32), gains[3:4]).astype(BF16)
    total = mixed.astype(F32)
    width = di_ref.shape[1]
    step = min(512, width)
    for at in range(0, width, step):
        inner = jax.nn.gelu(dot(normed_two, di_ref[:, at : at + step])).astype(BF16)
        total = total + dot(inner, do_ref[at : at + step, :])
    if windows > 1:
        total = dot(scatter, total.astype(BF16))
    return total


def whole_body(geo, x_hbm, k1_hbm, k2_hbm, mw_hbm, g_hbm, ai_hbm, ao_hbm, di_hbm, do_hbm, ew_hbm, ost,
               xv, k1_ref, k2_ref, mw_ref, g_ref, ai_ref, ao_ref, di_ref, do_ref, ew_ref,
               w1_ref, w2_ref, xs, xn, xf, fs, fn, ff, edges, sides, caps, corners,
               sbuf, rbuf, s2buf, r2buf, os,
               load_sem, halo_send, halo_recv, go_send, go_recv, back_send, back_recv):
    (nlat, nlon, bands, per_lon, offset_lat, offset_lon, pairs, joint, groups) = geo
    count = nlat * nlon
    lat = lax.axis_index("lat")
    lon = lax.axis_index("lon")
    me = lat * nlon + lon
    height, breadth, c = xv.shape
    half = breadth // 2
    latent = 4 * c
    tokens = bands * per_lon
    cells = bands * half
    reach = 2 * offset_lat
    rows = 2 * UNIT
    steps = offset_lat // UNIT
    block = UNIT * offset_lon // joint
    pitch = xs.shape[0] // (height + 4)

    head = EARLY_AT * rows - 2
    depth = rows + 4
    firsts = [pl.ds(p * reach + head, depth) for p in range(bands)]
    stops = [0] + [p * reach + head + depth for p in range(bands)]
    rests = [
        pl.ds(stop, (p * reach + head if p < bands else height) - stop) for p, stop in enumerate(stops)
    ]
    pieces = [(x_hbm.at[at], xv.at[at]) for at in firsts]
    pieces += [(k1_hbm, k1_ref), (k2_hbm, k2_ref), (mw_hbm, mw_ref)]
    pieces += [(x_hbm.at[at], xv.at[at]) for at in rests]
    pieces += [(g_hbm, g_ref), (ai_hbm, ai_ref), (ao_hbm, ao_ref), (di_hbm, di_ref), (do_hbm, do_ref), (ew_hbm, ew_ref)]
    loads = [pltpu.make_async_copy(a, b, load_sem.at[i]) for i, (a, b) in enumerate(pieces)]
    for load in loads:
        load.start()

    barrier = pltpu.get_barrier_semaphore()

    def greet(k, carry):
        peer = lax.rem(me + k, count)
        pl.semaphore_signal(
            barrier, inc=1, device_id=(lax.div(peer, nlon), lax.rem(peer, nlon)), device_id_type=MESH
        )
        return carry

    lax.fori_loop(1, count, greet, 0)

    def widen(r, carry):
        for k in range(4):
            at = 4 * r + k
            xs[pl.ds((at + 2) * pitch + LEAD, breadth), :] = xv[at].astype(F32)
        return carry

    def column(at):
        return xs[pl.ds(2 * pitch + LEAD + at, height, stride=pitch), :]

    left, right = LEAD - 2, LEAD + breadth
    for col in (left, left + 1, right, right + 1):
        xs[pl.ds(col, height + 4, stride=pitch), :] = jnp.zeros((height + 4, c), F32)

    for p in range(bands):
        loads[p].wait()
        for r in range(depth):
            at = p * reach + head + r
            xs[pl.ds((at + 2) * pitch + LEAD, breadth), :] = xv[at].astype(F32)
    loads[bands].wait()
    pair_kernel(k1_ref, w1_ref)
    loads[bands + 1].wait()
    pair_kernel(k2_ref, w2_ref)
    loads[bands + 2].wait()

    def fill(start, n):
        for r in range(n):
            base = (start + r) * pitch + left
            quad = [xs[pl.ds(base + j, pairs, stride=2), :] for j in range(4)]
            xn[pl.ds(start + r, 1)] = jnp.concatenate(quad[:2], axis=1).astype(BF16)[None]
            xf[pl.ds(start + r, 1)] = jnp.concatenate(quad[2:], axis=1).astype(BF16)[None]

    pair = lax.broadcasted_iota(jnp.int32, (pairs, 2 * c), 0)
    lane = lax.broadcasted_iota(jnp.int32, (pairs, 2 * c), 1)
    lon_place = 2 * pair + (lane >= c).astype(jnp.int32) + (lon * breadth - 1)
    inside = (lon_place >= 0) & (lon_place < nlon * breadth)

    def conv_one(starts, n):
        lhs = jnp.concatenate(
            [
                jnp.concatenate(
                    [buf[pl.ds(start + a, n)].reshape(n * pairs, 2 * c) for start in starts], axis=0
                )
                for a in range(3)
                for buf in (xn, xf)
            ],
            axis=1,
        )
        first = jax.nn.gelu(dot(lhs, w1_ref[...])).reshape(bands * n, pairs, 2 * c)
        fs[: bands * n] = jnp.where(inside[None], first, 0.0)
        for p, start in enumerate(starts):
            fn[pl.ds(start, n)] = fs[p * n : (p + 1) * n, 0:half, :].astype(BF16)
            ff[pl.ds(start, n)] = fs[p * n : (p + 1) * n, pl.ds(1, half), :].astype(BF16)

    to = lax.broadcasted_iota(jnp.int32, (cells, cells), 0)
    of = lax.broadcasted_iota(jnp.int32, (cells, cells), 1)
    outward = ones_where(of == (to % tokens) * offset_lon + to // tokens)
    inward = ones_where(of == (to % offset_lon) * tokens + to // offset_lon)

    span = offset_lon // joint
    nothing = jnp.zeros((1, half, 2 * c), BF16)

    def forward(entry, source):
        peer = lax.rem(entry, count)
        group = lax.div(entry, count)
        return pltpu.make_async_remote_copy(
            src_ref=sbuf.at[pl.ds(source, 1)], dst_ref=rbuf.at[pl.ds(group * count + me, 1)],
            send_sem=go_send.at[group], recv_sem=go_recv.at[group],
            device_id=(lax.div(peer, nlon), lax.rem(peer, nlon)), device_id_type=MESH,
        )

    def tail(base, place):
        lhs = jnp.concatenate(
            [
                jnp.concatenate(
                    [buf[pl.ds(start + a, rows)].reshape(rows * half, 2 * c) for start in base], axis=0
                )
                for a in range(3)
                for buf in (fn, ff)
            ],
            axis=1,
        )
        second = jax.nn.gelu(dot(lhs, w2_ref[...])).astype(BF16)
        second = second.reshape(bands * UNIT, 2, half, 2 * c)
        patches = jnp.concatenate(
            [second[:, d].reshape(bands * UNIT * half, 2 * c) for d in range(2)], axis=1
        )
        coarse = dot(patches, mw_ref[...]).astype(BF16).reshape(bands, UNIT, half, latent)
        for u in range(UNIT):
            moved = dot(outward, coarse[:, u].reshape(cells, latent))
            sbuf[pl.ds(place + u * span, span)] = moved.reshape(span, joint * tokens, latent).astype(BF16)


    def post(e, place, chosen):
        def send(k, carry):
            i = lax.rem(me + k, block)
            entry = e * block + i
            spot = lax.rem(i, span)
            take = chosen((spot == 0) | (spot == span - 1))
            mine = lax.rem(entry, count) == me

            @pl.when(take & jnp.logical_not(mine))
            def _():
                forward(entry, place + i).start()

            @pl.when(take & mine)
            def _():
                rbuf[pl.ds(entry, 1)] = sbuf[pl.ds(place + i, 1)]

            return carry

        lax.fori_loop(1, block + 1, send, 0)

    def early(j):
        e = EARLY_AT + j
        base = [p * reach + e * rows for p in range(bands)]
        for start in base:
            fill(start, rows + 4)
        conv_one(base, rows + 2)
        tail(base, (steps + j) * block)

    def early_post(j):
        post(EARLY_AT + j, (steps + j) * block, jnp.logical_not)

    early(0)
    pl.semaphore_wait(barrier, count - 1)
    early_post(0)

    for load in loads[bands + 3 : 2 * bands + 4]:
        load.wait()
    lax.fori_loop(0, height // 4, widen, 0)
    for side, at in enumerate((0, breadth - 2)):
        edges[side] = jnp.concatenate([column(at), column(at + 1)], axis=1).astype(BF16)

    tip = 16
    ends = (slice(0, tip), slice(height - tip, height))
    halo = []
    for i, (dy, dx) in enumerate(((-1, 0), (1, 0), (0, -1), (0, 1), (-1, -1), (-1, 1), (1, -1), (1, 1))):
        if dx == 0:
            src = xv.at[pl.ds(0 if dy < 0 else height - 2, 2)]
            dst = caps.at[1 if dy < 0 else 0]
        elif dy == 0:
            src = edges.at[0 if dx < 0 else 1]
            dst = sides.at[1 if dx < 0 else 0]
        else:
            first = 0 if dy < 0 else height - tip
            src = edges.at[0 if dx < 0 else 1, pl.ds(first, tip)]
            dst = corners.at[(2 if dy < 0 else 0) + (1 if dx < 0 else 0)]
        there = (lat + dy >= 0) & (lat + dy < nlat) & (lon + dx >= 0) & (lon + dx < nlon)
        back = (lat - dy >= 0) & (lat - dy < nlat) & (lon - dx >= 0) & (lon - dx < nlon)
        copy = pltpu.make_async_remote_copy(
            src_ref=src, dst_ref=dst, send_sem=halo_send.at[i], recv_sem=halo_recv.at[i],
            device_id=(jnp.clip(lat + dy, 0, nlat - 1), jnp.clip(lon + dx, 0, nlon - 1)), device_id_type=MESH,
        )
        halo.append((dy, dx, there, back, copy))
        pl.when(there)(copy.start)

    for j in range(1, EARLY):
        early(j)
        early_post(j)

    for dy, dx, there, back, copy in halo:
        row = 0 if dy > 0 else height + 2
        col = left if dx > 0 else right

        def landed(dy=dy, dx=dx, copy=copy, row=row, col=col):
            copy.wait_recv()
            if dx == 0:
                for k in range(2):
                    xs[pl.ds((row + k) * pitch + LEAD, breadth), :] = caps[0 if dy > 0 else 1, k].astype(F32)
            elif dy == 0:
                value = sides[0 if dx > 0 else 1].astype(F32)
                for k in range(2):
                    xs[pl.ds(2 * pitch + col + k, height, stride=pitch), :] = value[:, k * c : (k + 1) * c]
            else:
                value = corners[(0 if dy > 0 else 2) + (0 if dx > 0 else 1)].astype(F32)
                base = tip - 2 if dy > 0 else 0
                for r in range(2):
                    for k in range(2):
                        xs[pl.ds((row + r) * pitch + col + k, 1), :] = value[
                            base + r : base + r + 1, k * c : (k + 1) * c
                        ]

        def empty(row=row):
            for k in range(2):
                xs[pl.ds((row + k) * pitch + LEAD, breadth), :] = jnp.zeros((breadth, c), F32)

        pl.when(back)(landed)
        if dx == 0:
            pl.when(jnp.logical_not(back))(empty)

    def encode(k, carry):
        e = lax.rem(k + EARLY_AT + EARLY, steps)
        base = [p * reach + e * rows for p in range(bands)]

        @pl.when((k == 0) | (e == 0))
        def _():
            for start in base:
                fill(start, 4)
            conv_one(base, 2)

        @pl.when((lat == 0) & (e == 0))
        def _():
            fn[0:1] = nothing
            ff[0:1] = nothing

        for start in base:
            fill(start + 4, rows)
        conv_one([start + 2 for start in base], rows)

        @pl.when((lat == nlat - 1) & (e == steps - 1))
        def _():
            fn[height + 1 :] = nothing
            ff[height + 1 :] = nothing

        tail(base, e * block)
        fresh = (e < EARLY_AT) | (e >= EARLY_AT + EARLY)
        post(e, e * block, lambda edge: edge | fresh)
        return carry

    lax.fori_loop(0, steps, encode, 0)

    for load in loads[2 * bands + 4 :]:
        load.wait()

    def all_of(buffer, landing, send_sem, recv_sem, g):
        return pltpu.make_async_remote_copy(
            src_ref=buffer.at[pl.ds(0, count - 1)], dst_ref=landing.at[pl.ds(0, count - 1)],
            send_sem=send_sem.at[g], recv_sem=recv_sem.at[g],
            device_id=(lat, (lon + 1) % nlon), device_id_type=MESH,
        )

    per_group = steps // groups
    ahead = -(-(EARLY_AT + EARLY) // per_group)

    def attend(k, carry):
        g = lax.rem(k + ahead, groups)
        all_of(sbuf, rbuf, go_send, go_recv, g).wait_recv()
        at = pl.ds(g * count, count)
        cells_in = rbuf[at].astype(F32).reshape(count * joint * tokens, latent)
        total = window_block(joint, count, tokens, cells_in, g_ref, ai_ref, ao_ref, di_ref, do_ref)
        s2buf[at] = total.reshape(count, joint * tokens, latent).astype(BF16)

        def send(k, carry):
            peer = lax.rem(me + k, count)
            pltpu.make_async_remote_copy(
                src_ref=s2buf.at[pl.ds(g * count + peer, 1)], dst_ref=r2buf.at[pl.ds(g * count + me, 1)],
                send_sem=back_send.at[g], recv_sem=back_recv.at[g],
                device_id=(lax.div(peer, nlon), lax.rem(peer, nlon)), device_id_type=MESH,
            ).start()
            return carry

        lax.fori_loop(1, count, send, 0)
        own = pl.ds(g * count + me, 1)
        r2buf[own] = s2buf[own]
        return carry

    lax.fori_loop(0, groups, attend, 0)

    def expand(i, carry):
        g = lax.rem(i + ahead, groups)
        all_of(s2buf, r2buf, back_send, back_recv, g).wait_recv()
        for k in range(per_group):
            e = g * per_group + k
            placed = []
            for u in range(UNIT):
                got = r2buf[pl.ds(e * block + u * span, span)].astype(F32).reshape(cells, latent)
                placed.append(dot(inward, got.astype(BF16)).astype(BF16))
            made = dot(jnp.concatenate(placed, axis=0), ew_ref[...])
            for u in range(UNIT):
                for p in range(bands):
                    top = u * cells + p * half
                    for d in range(4):
                        line = (p * rows + 2 * u + d // 2) * breadth + d % 2
                        os[pl.ds(line, half, stride=2), :] = made[top : top + half, d * c : (d + 1) * c]
            for p in range(bands):
                place = pl.ds(p * reach + e * rows, rows)
                lines = os[p * rows * breadth : (p + 1) * rows * breadth, :].reshape(rows, breadth, c)
                ost[place] = (lines + xv[place].astype(F32)).astype(BF16)
        return carry

    lax.fori_loop(0, groups, expand, 0)

    def settle(g, carry):
        all_of(sbuf, rbuf, go_send, go_recv, g).wait_send()
        all_of(s2buf, r2buf, back_send, back_recv, g).wait_send()
        return carry

    lax.fori_loop(0, groups, settle, 0)
    for _, _, there, _, copy in halo:
        pl.when(there)(copy.wait_send)


def per_device(
    input_field,
    conv_one,
    conv_two,
    merge_weight,
    norm_gains,
    attention_in,
    attention_out,
    dense_in,
    dense_out,
    expand_weight,
):
    height, breadth, c = input_field.shape
    latent = merge_weight.shape[1]
    nlat = lax.axis_size("lat")
    nlon = lax.axis_size("lon")
    count = nlat * nlon
    bands = WINDOW // nlat
    per_lon = WINDOW // nlon
    offset_lat = height // (2 * bands)
    offset_lon = breadth // (2 * per_lon)
    tokens = bands * per_lon
    joint = max(1, 8 // tokens)
    entries = offset_lat * offset_lon // joint
    groups = entries // count
    half = breadth // 2
    pairs = -(-(half + 1) // 16) * 16
    pitch = -(-(LEAD + 2 * pairs) // 8) * 8
    rows = 2 * UNIT
    block = UNIT * offset_lon // joint
    args = (
        input_field, conv_one, conv_two, merge_weight, norm_gains,
        attention_in, attention_out, dense_in, dense_out, expand_weight,
    )
    geo = (nlat, nlon, bands, per_lon, offset_lat, offset_lon, pairs, joint, groups)
    message = (entries, joint * tokens, latent)
    scratch = [pltpu.VMEM(a.shape, a.dtype) for a in args]
    scratch += [
        pltpu.VMEM((12 * c, 2 * c), BF16),
        pltpu.VMEM((12 * c, 2 * c), BF16),
        pltpu.VMEM(((height + 4) * pitch, c), F32),
        pltpu.VMEM((height + 4, pairs, 2 * c), BF16),
        pltpu.VMEM((height + 4, pairs, 2 * c), BF16),
        pltpu.VMEM((bands * (rows + 2), pairs, 2 * c), F32),
        pltpu.VMEM((height + 2, half, 2 * c), BF16),
        pltpu.VMEM((height + 2, half, 2 * c), BF16),
        pltpu.VMEM((2, height, 2 * c), BF16),
        pltpu.VMEM((2, height, 2 * c), BF16),
        pltpu.VMEM((2, 2, breadth, c), BF16),
        pltpu.VMEM((4, 16, 2 * c), BF16),
        pltpu.VMEM((entries + EARLY * block,) + message[1:], BF16),
        pltpu.VMEM(message, BF16),
        pltpu.VMEM(message, BF16),
        pltpu.VMEM(message, BF16),
        pltpu.VMEM((bands * rows * breadth, c), F32),
        pltpu.SemaphoreType.DMA((2 * bands + 10,)),
        pltpu.SemaphoreType.DMA((8,)),
        pltpu.SemaphoreType.DMA((8,)),
        pltpu.SemaphoreType.DMA((groups,)),
        pltpu.SemaphoreType.DMA((groups,)),
        pltpu.SemaphoreType.DMA((groups,)),
        pltpu.SemaphoreType.DMA((groups,)),
    ]
    return pl.pallas_call(
        functools.partial(whole_body, geo),
        in_specs=[pl.BlockSpec(memory_space=pl.ANY)] * len(args),
        out_specs=pl.BlockSpec(memory_space=pltpu.VMEM),
        out_shape=pltpu.VMEM(input_field.shape, BF16),
        scratch_shapes=scratch,
        compiler_params=pltpu.CompilerParams(
            collective_id=0, has_side_effects=True, vmem_limit_bytes=LIMIT
        ),
        cost_estimate=pl.CostEstimate(flops=40_000_000_000, bytes_accessed=16_000_000, transcendentals=0),
        name="whole",
    )(*args)


def solution(mesh):
    return jax.shard_map(
        per_device,
        mesh=mesh,
        in_specs=(P("lat", "lon", None), P(), P(), P(), P(), P(), P(), P(), P(), P()),
        out_specs=P("lat", "lon", None),
        check_vma=False,
    )
```

```python
import functools
import math

import jax
import jax.numpy as jnp
from jax import lax
from jax.experimental import pallas as pl
from jax.experimental.pallas import tpu as pltpu
from jax.sharding import PartitionSpec as P

WINDOW = 16
HEAD_WIDTH = 32
EPSILON = 1e-06
FLOOR = 0.75
F32 = jnp.float32
BF16 = jnp.bfloat16
LIMIT = 56 * 1024 * 1024
MESH = pl.DeviceIdType.MESH
FLAT = pl.DeviceIdType.LOGICAL
LEAD = 8
UNIT = 2
EARLY = 2
EARLY_AT = 1


def dot(a, b):
    return jnp.dot(a, b, preferred_element_type=F32)


def ones_where(flag):
    return flag.astype(F32).astype(BF16)


def pair_kernel(kernel_ref, paired):
    taps, _, c, o = kernel_ref.shape
    zero = jnp.zeros((c, o), BF16)
    for a in range(taps):
        for b in range(4):
            rows = slice((4 * a + b) * c, (4 * a + b + 1) * c)
            paired[rows, :o] = kernel_ref[a, b] if b < 3 else zero
            paired[rows, o:] = kernel_ref[a, b - 1] if b > 0 else zero


def layer_norm(stream, gain):
    center = stream - jnp.mean(stream, axis=-1, keepdims=True)
    spread = jnp.mean(center * center, axis=-1, keepdims=True)
    return center * lax.rsqrt(spread + EPSILON) * gain


def window_block(windows, sources, tokens, cells, g_ref, ai_ref, ao_ref, di_ref, do_ref):
    latent = cells.shape[-1]
    size = sources * tokens
    count = windows * size
    coarse = cells
    if windows > 1:
        to = lax.broadcasted_iota(jnp.int32, (count, count), 0)
        of = lax.broadcasted_iota(jnp.int32, (count, count), 1)
        row = lax.broadcasted_iota(jnp.int32, (count, 1), 0)
        col = lax.broadcasted_iota(jnp.int32, (1, count), 1)

        def sorted_row(i):
            return (i // tokens % windows) * size + i // (tokens * windows) * tokens + i % tokens

        gather = ones_where(to == sorted_row(col))
        scatter = ones_where(of == sorted_row(row))
        coarse = dot(gather, cells.astype(BF16))
    gains = g_ref[...]
    normed = layer_norm(coarse, gains[0:1]).astype(BF16)
    head_row = lax.broadcasted_iota(jnp.int32, (latent, latent), 0) // HEAD_WIDTH
    head_col = lax.broadcasted_iota(jnp.int32, (latent, latent), 1) // HEAD_WIDTH
    spread = jnp.where(head_row == head_col, 1.0 / HEAD_WIDTH, 0.0).astype(BF16)

    def head_norm(stream, gain):
        square = dot((stream * stream).astype(BF16), spread)
        return (stream * gain * lax.rsqrt(jnp.maximum(square, FLOOR))).astype(BF16)

    queries = head_norm(dot(normed, ai_ref[:, :latent]), gains[1:2])
    key_rows = head_norm(dot(normed, ai_ref[:, latent : 2 * latent]), gains[2:3])
    values = dot(normed, ai_ref[:, 2 * latent :]).astype(BF16)
    group = 128
    heads = group // HEAD_WIDTH
    lane = lax.broadcasted_iota(jnp.int32, (size, group), 1) // HEAD_WIDTH
    marks = [ones_where(lane == h) for h in range(heads)]
    scale = HEAD_WIDTH ** (-0.5) * math.log2(math.e)
    parts = []
    for win in range(windows):
        span = slice(win * size, (win + 1) * size)
        row_parts = []
        for at in range(0, latent, group):
            q = queries[span, at : at + group]
            k = key_rows[span, at : at + group]
            v = values[span, at : at + group]
            expons = []
            stacked = []
            for h in range(heads):
                scores = lax.dot_general(
                    q * marks[h], k, (((1,), (1,)), ((), ())), preferred_element_type=F32
                )
                expons.append(jnp.exp2(scores * scale).astype(BF16))
                stacked.append(jnp.concatenate([v * marks[h], marks[h]], axis=1))
            both = dot(jnp.concatenate(expons, axis=1), jnp.concatenate(stacked, axis=0))
            row_parts.append((both[:, :group] / both[:, group:]).astype(BF16))
        parts.append(jnp.concatenate(row_parts, axis=1))
    attended = jnp.concatenate(parts, axis=0)
    mixed = (coarse + dot(attended, ao_ref[...])).astype(BF16)
    normed_two = layer_norm(mixed.astype(F32), gains[3:4]).astype(BF16)
    total = mixed.astype(F32)
    width = di_ref.shape[1]
    step = min(512, width)
    for at in range(0, width, step):
        inner = jax.nn.gelu(dot(normed_two, di_ref[:, at : at + step])).astype(BF16)
        total = total + dot(inner, do_ref[at : at + step, :])
    if windows > 1:
        total = dot(scatter, total.astype(BF16))
    return total


def whole_body(geo, x_hbm, k1_hbm, k2_hbm, mw_hbm, g_hbm, ai_hbm, ao_hbm, di_hbm, do_hbm, ew_hbm, ost,
               xv, k1_ref, k2_ref, mw_ref, g_ref, ai_ref, ao_ref, di_ref, do_ref, ew_ref,
               w1_ref, w2_ref, xs, xn, xf, fs, fn, ff, edges, sides, caps, corners,
               sbuf, rbuf, s2buf, r2buf, os,
               load_sem, halo_send, halo_recv, go_send, go_recv, back_send, back_recv):
    (nlat, nlon, bands, per_lon, offset_lat, offset_lon, pairs, joint, groups) = geo
    count = nlat * nlon
    lat = lax.axis_index("lat")
    lon = lax.axis_index("lon")
    me = lat * nlon + lon
    height, breadth, c = xv.shape
    half = breadth // 2
    latent = 4 * c
    tokens = bands * per_lon
    cells = bands * half
    reach = 2 * offset_lat
    rows = 2 * UNIT
    steps = offset_lat // UNIT
    block = UNIT * offset_lon // joint
    pitch = xs.shape[0] // (height + 4)

    head = EARLY_AT * rows - 2
    depth = rows + 4
    firsts = [pl.ds(p * reach + head, depth) for p in range(bands)]
    stops = [0] + [p * reach + head + depth for p in range(bands)]
    rests = [
        pl.ds(stop, (p * reach + head if p < bands else height) - stop) for p, stop in enumerate(stops)
    ]
    pieces = [(x_hbm.at[at], xv.at[at]) for at in firsts]
    pieces += [(k1_hbm, k1_ref), (k2_hbm, k2_ref), (mw_hbm, mw_ref)]
    pieces += [(x_hbm.at[at], xv.at[at]) for at in rests]
    pieces += [(g_hbm, g_ref), (ai_hbm, ai_ref), (ao_hbm, ao_ref), (di_hbm, di_ref), (do_hbm, do_ref), (ew_hbm, ew_ref)]
    loads = [pltpu.make_async_copy(a, b, load_sem.at[i]) for i, (a, b) in enumerate(pieces)]
    for load in loads:
        load.start()

    barrier = pltpu.get_barrier_semaphore()

    def greet(k, carry):
        pl.semaphore_signal(barrier, inc=1, device_id=lax.rem(me + k, count), device_id_type=FLAT)
        return carry

    lax.fori_loop(1, count, greet, 0)

    def widen(r, carry):
        for k in range(4):
            at = 4 * r + k
            xs[pl.ds((at + 2) * pitch + LEAD, breadth), :] = xv[at].astype(F32)
        return carry

    def column(at):
        return xs[pl.ds(2 * pitch + LEAD + at, height, stride=pitch), :]

    left, right = LEAD - 2, LEAD + breadth
    for col in (left, left + 1, right, right + 1):
        xs[pl.ds(col, height + 4, stride=pitch), :] = jnp.zeros((height + 4, c), F32)

    for p in range(bands):
        loads[p].wait()
        for r in range(depth):
            at = p * reach + head + r
            xs[pl.ds((at + 2) * pitch + LEAD, breadth), :] = xv[at].astype(F32)
    loads[bands].wait()
    pair_kernel(k1_ref, w1_ref)
    loads[bands + 1].wait()
    pair_kernel(k2_ref, w2_ref)
    loads[bands + 2].wait()

    def fill(start, n):
        for r in range(n):
            base = (start + r) * pitch + left
            quad = [xs[pl.ds(base + j, pairs, stride=2), :] for j in range(4)]
            xn[pl.ds(start + r, 1)] = jnp.concatenate(quad[:2], axis=1).astype(BF16)[None]
            xf[pl.ds(start + r, 1)] = jnp.concatenate(quad[2:], axis=1).astype(BF16)[None]

    pair = lax.broadcasted_iota(jnp.int32, (pairs, 2 * c), 0)
    lane = lax.broadcasted_iota(jnp.int32, (pairs, 2 * c), 1)
    lon_place = 2 * pair + (lane >= c).astype(jnp.int32) + (lon * breadth - 1)
    inside = (lon_place >= 0) & (lon_place < nlon * breadth)

    def conv_one(starts, n):
        lhs = jnp.concatenate(
            [
                jnp.concatenate(
                    [buf[pl.ds(start + a, n)].reshape(n * pairs, 2 * c) for start in starts], axis=0
                )
                for a in range(3)
                for buf in (xn, xf)
            ],
            axis=1,
        )
        first = jax.nn.gelu(dot(lhs, w1_ref[...])).reshape(bands * n, pairs, 2 * c)
        fs[: bands * n] = jnp.where(inside[None], first, 0.0)
        for p, start in enumerate(starts):
            fn[pl.ds(start, n)] = fs[p * n : (p + 1) * n, 0:half, :].astype(BF16)
            ff[pl.ds(start, n)] = fs[p * n : (p + 1) * n, pl.ds(1, half), :].astype(BF16)

    to = lax.broadcasted_iota(jnp.int32, (cells, cells), 0)
    of = lax.broadcasted_iota(jnp.int32, (cells, cells), 1)
    outward = ones_where(of == (to % tokens) * offset_lon + to // tokens)
    inward = ones_where(of == (to % offset_lon) * tokens + to // offset_lon)

    span = offset_lon // joint
    nothing = jnp.zeros((1, half, 2 * c), BF16)

    def tail(base, place, units):
        lines = 2 * units
        lhs = jnp.concatenate(
            [
                jnp.concatenate(
                    [buf[pl.ds(start + a, lines)].reshape(lines * half, 2 * c) for start in base], axis=0
                )
                for a in range(3)
                for buf in (fn, ff)
            ],
            axis=1,
        )
        second = jax.nn.gelu(dot(lhs, w2_ref[...])).astype(BF16)
        second = second.reshape(bands * units, 2, half, 2 * c)
        patches = jnp.concatenate(
            [second[:, d].reshape(bands * units * half, 2 * c) for d in range(2)], axis=1
        )
        coarse = dot(patches, mw_ref[...]).astype(BF16).reshape(bands, units, half, latent)
        for u in range(units):
            moved = dot(outward, coarse[:, u].reshape(cells, latent))
            sbuf[pl.ds(place + u * span, span)] = moved.reshape(span, joint * tokens, latent).astype(BF16)


    def post(e, place, low, n, chosen):
        def send(k, carry):
            i = low + lax.rem(me + k, n)
            entry = e * block + i
            peer = i if block == count else lax.rem(entry, count)
            group = e if block == count else lax.div(entry, count)
            spot = lax.rem(i, span)
            take = chosen((spot == 0) | (spot == span - 1))

            @pl.when(take & (peer != me))
            def _():
                pltpu.make_async_remote_copy(
                    src_ref=sbuf.at[pl.ds(place + i, 1)], dst_ref=rbuf.at[pl.ds(group * count + me, 1)],
                    send_sem=go_send.at[group], recv_sem=go_recv.at[group],
                    device_id=peer, device_id_type=FLAT,
                ).start()

            @pl.when(take & (peer == me))
            def _():
                rbuf[pl.ds(entry, 1)] = sbuf[pl.ds(place + i, 1)]

            return carry

        lax.fori_loop(1, n + 1, send, 0)

    def early(j, low, units):
        e = EARLY_AT + j
        base = [p * reach + e * rows + 2 * low for p in range(bands)]
        fresh = j == 0 and low == 0
        more = 2 if fresh else 0
        for start in base:
            fill(start + 4 - 2 * more, 2 * units + 2 * more)
        conv_one([start + 2 - more for start in base], 2 * units + more)
        tail(base, (steps + j) * block + low * span, units)

    def early_post(j, low, units):
        post(EARLY_AT + j, (steps + j) * block, low * span, units * span, jnp.logical_not)

    early(0, 0, 1)
    pl.semaphore_wait(barrier, count - 1)
    early_post(0, 0, 1)
    for low in range(1, UNIT):
        early(0, low, 1)
        early_post(0, low, 1)

    for load in loads[bands + 3 : 2 * bands + 4]:
        load.wait()
    lax.fori_loop(0, height // 4, widen, 0)
    for side, at in enumerate((0, breadth - 2)):
        edges[side] = jnp.concatenate([column(at), column(at + 1)], axis=1).astype(BF16)

    tip = 16
    ends = (slice(0, tip), slice(height - tip, height))
    halo = []
    for i, (dy, dx) in enumerate(((-1, 0), (1, 0), (0, -1), (0, 1), (-1, -1), (-1, 1), (1, -1), (1, 1))):
        if dx == 0:
            src = xv.at[pl.ds(0 if dy < 0 else height - 2, 2)]
            dst = caps.at[1 if dy < 0 else 0]
        elif dy == 0:
            src = edges.at[0 if dx < 0 else 1]
            dst = sides.at[1 if dx < 0 else 0]
        else:
            first = 0 if dy < 0 else height - tip
            src = edges.at[0 if dx < 0 else 1, pl.ds(first, tip)]
            dst = corners.at[(2 if dy < 0 else 0) + (1 if dx < 0 else 0)]
        there = (lat + dy >= 0) & (lat + dy < nlat) & (lon + dx >= 0) & (lon + dx < nlon)
        back = (lat - dy >= 0) & (lat - dy < nlat) & (lon - dx >= 0) & (lon - dx < nlon)
        copy = pltpu.make_async_remote_copy(
            src_ref=src, dst_ref=dst, send_sem=halo_send.at[i], recv_sem=halo_recv.at[i],
            device_id=(jnp.clip(lat + dy, 0, nlat - 1), jnp.clip(lon + dx, 0, nlon - 1)), device_id_type=MESH,
        )
        halo.append((dy, dx, there, back, copy))
        pl.when(there)(copy.start)

    for j in range(1, EARLY):
        early(j, 0, UNIT)
        early_post(j, 0, UNIT)

    for dy, dx, there, back, copy in halo:
        row = 0 if dy > 0 else height + 2
        col = left if dx > 0 else right

        def landed(dy=dy, dx=dx, copy=copy, row=row, col=col):
            copy.wait_recv()
            if dx == 0:
                for k in range(2):
                    xs[pl.ds((row + k) * pitch + LEAD, breadth), :] = caps[0 if dy > 0 else 1, k].astype(F32)
            elif dy == 0:
                value = sides[0 if dx > 0 else 1].astype(F32)
                for k in range(2):
                    xs[pl.ds(2 * pitch + col + k, height, stride=pitch), :] = value[:, k * c : (k + 1) * c]
            else:
                value = corners[(0 if dy > 0 else 2) + (0 if dx > 0 else 1)].astype(F32)
                base = tip - 2 if dy > 0 else 0
                for r in range(2):
                    for k in range(2):
                        xs[pl.ds((row + r) * pitch + col + k, 1), :] = value[
                            base + r : base + r + 1, k * c : (k + 1) * c
                        ]

        def empty(row=row):
            for k in range(2):
                xs[pl.ds((row + k) * pitch + LEAD, breadth), :] = jnp.zeros((breadth, c), F32)

        pl.when(back)(landed)
        if dx == 0:
            pl.when(jnp.logical_not(back))(empty)

    def encode(k, carry):
        e = lax.rem(k + EARLY_AT + EARLY, steps)
        base = [p * reach + e * rows for p in range(bands)]

        @pl.when((k == 0) | (e == 0))
        def _():
            for start in base:
                fill(start, 4)
            conv_one(base, 2)

        @pl.when((lat == 0) & (e == 0))
        def _():
            fn[0:1] = nothing
            ff[0:1] = nothing

        for start in base:
            fill(start + 4, rows)
        conv_one([start + 2 for start in base], rows)

        @pl.when((lat == nlat - 1) & (e == steps - 1))
        def _():
            fn[height + 1 :] = nothing
            ff[height + 1 :] = nothing

        tail(base, e * block, UNIT)
        fresh = (e < EARLY_AT) | (e >= EARLY_AT + EARLY)
        post(e, e * block, 0, block, lambda edge: edge | fresh)
        return carry

    lax.fori_loop(0, steps, encode, 0)

    for load in loads[2 * bands + 4 :]:
        load.wait()

    def all_of(buffer, landing, send_sem, recv_sem, g):
        return pltpu.make_async_remote_copy(
            src_ref=buffer.at[pl.ds(0, count - 1)], dst_ref=landing.at[pl.ds(0, count - 1)],
            send_sem=send_sem.at[g], recv_sem=recv_sem.at[g],
            device_id=(lat, (lon + 1) % nlon), device_id_type=MESH,
        )

    per_group = steps // groups
    ahead = -(-(EARLY_AT + EARLY) // per_group)

    def attend(k, carry):
        g = lax.rem(k + ahead, groups)
        all_of(sbuf, rbuf, go_send, go_recv, g).wait_recv()
        at = pl.ds(g * count, count)
        cells_in = rbuf[at].astype(F32).reshape(count * joint * tokens, latent)
        total = window_block(joint, count, tokens, cells_in, g_ref, ai_ref, ao_ref, di_ref, do_ref)
        s2buf[at] = total.reshape(count, joint * tokens, latent).astype(BF16)

        def send(k, carry):
            peer = lax.rem(me + k, count)
            pltpu.make_async_remote_copy(
                src_ref=s2buf.at[pl.ds(g * count + peer, 1)], dst_ref=r2buf.at[pl.ds(g * count + me, 1)],
                send_sem=back_send.at[g], recv_sem=back_recv.at[g],
                device_id=peer, device_id_type=FLAT,
            ).start()
            return carry

        lax.fori_loop(1, count, send, 0)
        own = pl.ds(g * count + me, 1)
        r2buf[own] = s2buf[own]
        return carry

    lax.fori_loop(0, groups, attend, 0)

    def expand(i, carry):
        g = lax.rem(i + ahead, groups)
        all_of(s2buf, r2buf, back_send, back_recv, g).wait_recv()
        for k in range(per_group):
            e = g * per_group + k
            placed = []
            for u in range(UNIT):
                got = r2buf[pl.ds(e * block + u * span, span)].astype(F32).reshape(cells, latent)
                placed.append(dot(inward, got.astype(BF16)).astype(BF16))
            made = dot(jnp.concatenate(placed, axis=0), ew_ref[...])
            for u in range(UNIT):
                for p in range(bands):
                    top = u * cells + p * half
                    for d in range(4):
                        line = (p * rows + 2 * u + d // 2) * breadth + d % 2
                        os[pl.ds(line, half, stride=2), :] = made[top : top + half, d * c : (d + 1) * c]
            for p in range(bands):
                place = pl.ds(p * reach + e * rows, rows)
                lines = os[p * rows * breadth : (p + 1) * rows * breadth, :].reshape(rows, breadth, c)
                ost[place] = (lines + xv[place].astype(F32)).astype(BF16)
        return carry

    lax.fori_loop(0, groups, expand, 0)

    def settle(g, carry):
        all_of(sbuf, rbuf, go_send, go_recv, g).wait_send()
        all_of(s2buf, r2buf, back_send, back_recv, g).wait_send()
        return carry

    lax.fori_loop(0, groups, settle, 0)
    for _, _, there, _, copy in halo:
        pl.when(there)(copy.wait_send)


def per_device(
    input_field,
    conv_one,
    conv_two,
    merge_weight,
    norm_gains,
    attention_in,
    attention_out,
    dense_in,
    dense_out,
    expand_weight,
):
    height, breadth, c = input_field.shape
    latent = merge_weight.shape[1]
    nlat = lax.axis_size("lat")
    nlon = lax.axis_size("lon")
    count = nlat * nlon
    bands = WINDOW // nlat
    per_lon = WINDOW // nlon
    offset_lat = height // (2 * bands)
    offset_lon = breadth // (2 * per_lon)
    tokens = bands * per_lon
    joint = max(1, 8 // tokens)
    entries = offset_lat * offset_lon // joint
    groups = entries // count
    half = breadth // 2
    pairs = -(-(half + 1) // 16) * 16
    pitch = -(-(LEAD + 2 * pairs) // 8) * 8
    rows = 2 * UNIT
    block = UNIT * offset_lon // joint
    args = (
        input_field, conv_one, conv_two, merge_weight, norm_gains,
        attention_in, attention_out, dense_in, dense_out, expand_weight,
    )
    geo = (nlat, nlon, bands, per_lon, offset_lat, offset_lon, pairs, joint, groups)
    message = (entries, joint * tokens, latent)
    scratch = [pltpu.VMEM(a.shape, a.dtype) for a in args]
    scratch += [
        pltpu.VMEM((12 * c, 2 * c), BF16),
        pltpu.VMEM((12 * c, 2 * c), BF16),
        pltpu.VMEM(((height + 4) * pitch, c), F32),
        pltpu.VMEM((height + 4, pairs, 2 * c), BF16),
        pltpu.VMEM((height + 4, pairs, 2 * c), BF16),
        pltpu.VMEM((bands * (rows + 2), pairs, 2 * c), F32),
        pltpu.VMEM((height + 2, half, 2 * c), BF16),
        pltpu.VMEM((height + 2, half, 2 * c), BF16),
        pltpu.VMEM((2, height, 2 * c), BF16),
        pltpu.VMEM((2, height, 2 * c), BF16),
        pltpu.VMEM((2, 2, breadth, c), BF16),
        pltpu.VMEM((4, 16, 2 * c), BF16),
        pltpu.VMEM((entries + EARLY * block,) + message[1:], BF16),
        pltpu.VMEM(message, BF16),
        pltpu.VMEM(message, BF16),
        pltpu.VMEM(message, BF16),
        pltpu.VMEM((bands * rows * breadth, c), F32),
        pltpu.SemaphoreType.DMA((2 * bands + 10,)),
        pltpu.SemaphoreType.DMA((8,)),
        pltpu.SemaphoreType.DMA((8,)),
        pltpu.SemaphoreType.DMA((groups,)),
        pltpu.SemaphoreType.DMA((groups,)),
        pltpu.SemaphoreType.DMA((groups,)),
        pltpu.SemaphoreType.DMA((groups,)),
    ]
    return pl.pallas_call(
        functools.partial(whole_body, geo),
        in_specs=[pl.BlockSpec(memory_space=pl.ANY)] * len(args),
        out_specs=pl.BlockSpec(memory_space=pltpu.VMEM),
        out_shape=pltpu.VMEM(input_field.shape, BF16),
        scratch_shapes=scratch,
        compiler_params=pltpu.CompilerParams(
            collective_id=0, has_side_effects=True, vmem_limit_bytes=LIMIT
        ),
        cost_estimate=pl.CostEstimate(flops=40_000_000_000, bytes_accessed=16_000_000, transcendentals=0),
        name="whole",
    )(*args)


def solution(mesh):
    return jax.shard_map(
        per_device,
        mesh=mesh,
        in_specs=(P("lat", "lon", None), P(), P(), P(), P(), P(), P(), P(), P(), P()),
        out_specs=P("lat", "lon", None),
        check_vma=False,
    )
```

```python
import functools
import math

import jax
import jax.numpy as jnp
from jax import lax
from jax.experimental import pallas as pl
from jax.experimental.pallas import tpu as pltpu
from jax.sharding import PartitionSpec as P

WINDOW = 16
HEAD_WIDTH = 32
EPSILON = 1e-06
FLOOR = 0.75
F32 = jnp.float32
BF16 = jnp.bfloat16
LIMIT = 56 * 1024 * 1024
MESH = pl.DeviceIdType.MESH
FLAT = pl.DeviceIdType.LOGICAL
LEAD = 8
UNIT = 2
FLUSHES = 8
EARLY = 2
EARLY_AT = 1


def dot(a, b):
    return jnp.dot(a, b, preferred_element_type=F32)


def ones_where(flag):
    return flag.astype(F32).astype(BF16)


def pair_kernel(kernel_ref, paired):
    taps, _, c, o = kernel_ref.shape
    zero = jnp.zeros((c, o), BF16)
    for a in range(taps):
        for b in range(4):
            rows = slice((4 * a + b) * c, (4 * a + b + 1) * c)
            paired[rows, :o] = kernel_ref[a, b] if b < 3 else zero
            paired[rows, o:] = kernel_ref[a, b - 1] if b > 0 else zero


def layer_norm(stream, gain):
    center = stream - jnp.mean(stream, axis=-1, keepdims=True)
    spread = jnp.mean(center * center, axis=-1, keepdims=True)
    return center * lax.rsqrt(spread + EPSILON) * gain


def window_block(windows, sources, tokens, cells, g_ref, ai_ref, ao_ref, di_ref, do_ref):
    latent = cells.shape[-1]
    size = sources * tokens
    count = windows * size
    coarse = cells
    if windows > 1:
        to = lax.broadcasted_iota(jnp.int32, (count, count), 0)
        of = lax.broadcasted_iota(jnp.int32, (count, count), 1)
        row = lax.broadcasted_iota(jnp.int32, (count, 1), 0)
        col = lax.broadcasted_iota(jnp.int32, (1, count), 1)

        def sorted_row(i):
            return (i // tokens % windows) * size + i // (tokens * windows) * tokens + i % tokens

        gather = ones_where(to == sorted_row(col))
        scatter = ones_where(of == sorted_row(row))
        coarse = dot(gather, cells.astype(BF16))
    gains = g_ref[...]
    normed = layer_norm(coarse, gains[0:1]).astype(BF16)
    head_row = lax.broadcasted_iota(jnp.int32, (latent, latent), 0) // HEAD_WIDTH
    head_col = lax.broadcasted_iota(jnp.int32, (latent, latent), 1) // HEAD_WIDTH
    spread = jnp.where(head_row == head_col, 1.0 / HEAD_WIDTH, 0.0).astype(BF16)

    def head_norm(stream, gain):
        square = dot((stream * stream).astype(BF16), spread)
        return (stream * gain * lax.rsqrt(jnp.maximum(square, FLOOR))).astype(BF16)

    queries = head_norm(dot(normed, ai_ref[:, :latent]), gains[1:2])
    key_rows = head_norm(dot(normed, ai_ref[:, latent : 2 * latent]), gains[2:3])
    values = dot(normed, ai_ref[:, 2 * latent :]).astype(BF16)
    group = 128
    heads = group // HEAD_WIDTH
    lane = lax.broadcasted_iota(jnp.int32, (size, group), 1) // HEAD_WIDTH
    marks = [ones_where(lane == h) for h in range(heads)]
    scale = HEAD_WIDTH ** (-0.5) * math.log2(math.e)
    parts = []
    for win in range(windows):
        span = slice(win * size, (win + 1) * size)
        row_parts = []
        for at in range(0, latent, group):
            q = queries[span, at : at + group]
            k = key_rows[span, at : at + group]
            v = values[span, at : at + group]
            expons = []
            stacked = []
            for h in range(heads):
                scores = lax.dot_general(
                    q * marks[h], k, (((1,), (1,)), ((), ())), preferred_element_type=F32
                )
                expons.append(jnp.exp2(scores * scale).astype(BF16))
                stacked.append(jnp.concatenate([v * marks[h], marks[h]], axis=1))
            both = dot(jnp.concatenate(expons, axis=1), jnp.concatenate(stacked, axis=0))
            row_parts.append((both[:, :group] / both[:, group:]).astype(BF16))
        parts.append(jnp.concatenate(row_parts, axis=1))
    attended = jnp.concatenate(parts, axis=0)
    mixed = (coarse + dot(attended, ao_ref[...])).astype(BF16)
    normed_two = layer_norm(mixed.astype(F32), gains[3:4]).astype(BF16)
    total = mixed.astype(F32)
    width = di_ref.shape[1]
    step = min(512, width)
    for at in range(0, width, step):
        inner = jax.nn.gelu(dot(normed_two, di_ref[:, at : at + step])).astype(BF16)
        total = total + dot(inner, do_ref[at : at + step, :])
    if windows > 1:
        total = dot(scatter, total.astype(BF16))
    return total


def whole_body(geo, x_hbm, k1_hbm, k2_hbm, mw_hbm, g_hbm, ai_hbm, ao_hbm, di_hbm, do_hbm, ew_hbm, ost,
               xv, k1_ref, k2_ref, mw_ref, g_ref, ai_ref, ao_ref, di_ref, do_ref, ew_ref,
               w1_ref, w2_ref, xs, xn, xf, fs, fn, ff, edges, sides, caps, corners,
               sbuf, rbuf, s2buf, r2buf, os,
               load_sem, halo_send, halo_recv, go_send, go_recv, back_send, back_recv):
    (nlat, nlon, bands, per_lon, offset_lat, offset_lon, pairs, joint, groups) = geo
    count = nlat * nlon
    lat = lax.axis_index("lat")
    lon = lax.axis_index("lon")
    me = lat * nlon + lon
    height, breadth, c = xv.shape
    half = breadth // 2
    latent = 4 * c
    tokens = bands * per_lon
    cells = bands * half
    reach = 2 * offset_lat
    rows = 2 * UNIT
    steps = offset_lat // UNIT
    block = UNIT * offset_lon // joint
    pitch = xs.shape[0] // (height + 5)

    head = EARLY_AT * rows - 2
    depth = rows + 4
    firsts = [pl.ds(p * reach + head, depth) for p in range(bands)]
    stops = [0] + [p * reach + head + depth for p in range(bands)]
    rests = [
        pl.ds(stop, (p * reach + head if p < bands else height) - stop) for p, stop in enumerate(stops)
    ]
    pieces = [(x_hbm.at[at], xv.at[at]) for at in firsts]
    pieces += [(k1_hbm, k1_ref), (k2_hbm, k2_ref), (mw_hbm, mw_ref)]
    pieces += [(x_hbm.at[at], xv.at[at]) for at in rests]
    pieces += [(g_hbm, g_ref), (ai_hbm, ai_ref), (ao_hbm, ao_ref), (di_hbm, di_ref), (do_hbm, do_ref), (ew_hbm, ew_ref)]
    loads = [pltpu.make_async_copy(a, b, load_sem.at[i]) for i, (a, b) in enumerate(pieces)]
    for load in loads:
        load.start()

    barrier = pltpu.get_barrier_semaphore()

    def greet(k, carry):
        pl.semaphore_signal(barrier, inc=1, device_id=lax.rem(me + k, count), device_id_type=FLAT)
        return carry

    lax.fori_loop(1, count, greet, 0)

    def widen(r, carry):
        for k in range(4):
            at = 4 * r + k
            xs[pl.ds((at + 2) * pitch + LEAD, breadth), :] = xv[at].astype(F32)
        return carry

    def column(at):
        return xs[pl.ds(2 * pitch + LEAD + at, height, stride=pitch), :]

    left, right = LEAD - 2, LEAD + breadth
    for col in (left, left + 1, right, right + 1):
        xs[pl.ds(col, height + 4, stride=pitch), :] = jnp.zeros((height + 4, c), F32)

    for p in range(bands):
        loads[p].wait()
        for r in range(depth):
            at = p * reach + head + r
            xs[pl.ds((at + 2) * pitch + LEAD, breadth), :] = xv[at].astype(F32)
    loads[bands].wait()
    pair_kernel(k1_ref, w1_ref)
    loads[bands + 1].wait()
    pair_kernel(k2_ref, w2_ref)
    loads[bands + 2].wait()

    def fill(start, n):
        for r in range(n):
            base = (start + r) * pitch + left
            quad = [xs[pl.ds(base + j, pairs, stride=2), :] for j in range(4)]
            xn[pl.ds(start + r, 1)] = jnp.concatenate(quad[:2], axis=1).astype(BF16)[None]
            xf[pl.ds(start + r, 1)] = jnp.concatenate(quad[2:], axis=1).astype(BF16)[None]

    pair = lax.broadcasted_iota(jnp.int32, (pairs, 2 * c), 0)
    lane = lax.broadcasted_iota(jnp.int32, (pairs, 2 * c), 1)
    lon_place = 2 * pair + (lane >= c).astype(jnp.int32) + (lon * breadth - 1)
    inside = (lon_place >= 0) & (lon_place < nlon * breadth)

    def conv_one(starts, n):
        lhs = jnp.concatenate(
            [
                jnp.concatenate(
                    [buf[pl.ds(start + a, n)].reshape(n * pairs, 2 * c) for start in starts], axis=0
                )
                for a in range(3)
                for buf in (xn, xf)
            ],
            axis=1,
        )
        first = jax.nn.gelu(dot(lhs, w1_ref[...])).reshape(bands * n, pairs, 2 * c)
        fs[: bands * n] = jnp.where(inside[None], first, 0.0)
        for p, start in enumerate(starts):
            fn[pl.ds(start, n)] = fs[p * n : (p + 1) * n, 0:half, :].astype(BF16)
            ff[pl.ds(start, n)] = fs[p * n : (p + 1) * n, pl.ds(1, half), :].astype(BF16)

    to = lax.broadcasted_iota(jnp.int32, (cells, cells), 0)
    of = lax.broadcasted_iota(jnp.int32, (cells, cells), 1)
    outward = ones_where(of == (to % tokens) * offset_lon + to // tokens)
    inward = ones_where(of == (to % offset_lon) * tokens + to // offset_lon)

    span = offset_lon // joint
    nothing = jnp.zeros((1, half, 2 * c), BF16)

    def tail(base, place, units):
        lines = 2 * units
        lhs = jnp.concatenate(
            [
                jnp.concatenate(
                    [buf[pl.ds(start + a, lines)].reshape(lines * half, 2 * c) for start in base], axis=0
                )
                for a in range(3)
                for buf in (fn, ff)
            ],
            axis=1,
        )
        second = jax.nn.gelu(dot(lhs, w2_ref[...])).astype(BF16)
        second = second.reshape(bands * units, 2, half, 2 * c)
        patches = jnp.concatenate(
            [second[:, d].reshape(bands * units * half, 2 * c) for d in range(2)], axis=1
        )
        coarse = dot(patches, mw_ref[...]).astype(BF16).reshape(bands, units, half, latent)
        for u in range(units):
            moved = dot(outward, coarse[:, u].reshape(cells, latent))
            sbuf[pl.ds(place + u * span, span)] = moved.reshape(span, joint * tokens, latent).astype(BF16)


    def post(e, place, low, n, chosen):
        def send(k, carry):
            i = low + lax.rem(me + k, n)
            entry = e * block + i
            peer = i if block == count else lax.rem(entry, count)
            group = e if block == count else lax.div(entry, count)
            spot = lax.rem(i, span)
            take = chosen((spot == 0) | (spot == span - 1))

            @pl.when(take & (peer != me))
            def _():
                pltpu.make_async_remote_copy(
                    src_ref=sbuf.at[pl.ds(place + i, 1)], dst_ref=rbuf.at[pl.ds(group * count + me, 1)],
                    send_sem=go_send.at[group], recv_sem=go_recv.at[group],
                    device_id=peer, device_id_type=FLAT,
                ).start()

            @pl.when(take & (peer == me))
            def _():
                rbuf[pl.ds(entry, 1)] = sbuf[pl.ds(place + i, 1)]

            return carry

        lax.fori_loop(1, n + 1, send, 0)

    def early(j, low, units):
        e = EARLY_AT + j
        base = [p * reach + e * rows + 2 * low for p in range(bands)]
        fresh = j == 0 and low == 0
        more = 2 if fresh else 0
        for start in base:
            fill(start + 4 - 2 * more, 2 * units + 2 * more)
        conv_one([start + 2 - more for start in base], 2 * units + more)
        tail(base, (steps + j) * block + low * span, units)

    def early_post(j, low, units):
        post(EARLY_AT + j, (steps + j) * block, low * span, units * span, jnp.logical_not)

    early(0, 0, 1)
    pl.semaphore_wait(barrier, count - 1)
    early_post(0, 0, 1)
    for low in range(1, UNIT):
        early(0, low, 1)
        early_post(0, low, 1)

    for load in loads[bands + 3 : 2 * bands + 4]:
        load.wait()
    lax.fori_loop(0, height // 4, widen, 0)
    for side, at in enumerate((0, breadth - 2)):
        edges[side] = jnp.concatenate([column(at), column(at + 1)], axis=1).astype(BF16)

    tip = 16
    ends = (slice(0, tip), slice(height - tip, height))
    halo = []
    for i, (dy, dx) in enumerate(((-1, 0), (1, 0), (0, -1), (0, 1), (-1, -1), (-1, 1), (1, -1), (1, 1))):
        if dx == 0:
            src = xv.at[pl.ds(0 if dy < 0 else height - 2, 2)]
            dst = caps.at[1 if dy < 0 else 0]
        elif dy == 0:
            src = edges.at[0 if dx < 0 else 1]
            dst = sides.at[1 if dx < 0 else 0]
        else:
            first = 0 if dy < 0 else height - tip
            src = edges.at[0 if dx < 0 else 1, pl.ds(first, tip)]
            dst = corners.at[(2 if dy < 0 else 0) + (1 if dx < 0 else 0)]
        there = (lat + dy >= 0) & (lat + dy < nlat) & (lon + dx >= 0) & (lon + dx < nlon)
        back = (lat - dy >= 0) & (lat - dy < nlat) & (lon - dx >= 0) & (lon - dx < nlon)
        copy = pltpu.make_async_remote_copy(
            src_ref=src, dst_ref=dst, send_sem=halo_send.at[i], recv_sem=halo_recv.at[i],
            device_id=(jnp.clip(lat + dy, 0, nlat - 1), jnp.clip(lon + dx, 0, nlon - 1)), device_id_type=MESH,
        )
        halo.append((dy, dx, there, back, copy))
        pl.when(there)(copy.start)

    for j in range(1, EARLY):
        early(j, 0, UNIT)
        early_post(j, 0, UNIT)

    for dy, dx, there, back, copy in halo:
        row = 0 if dy > 0 else height + 2
        col = left if dx > 0 else right

        def landed(dy=dy, dx=dx, copy=copy, row=row, col=col):
            copy.wait_recv()
            if dx == 0:
                for k in range(2):
                    xs[pl.ds((row + k) * pitch + LEAD, breadth), :] = caps[0 if dy > 0 else 1, k].astype(F32)
            elif dy == 0:
                value = sides[0 if dx > 0 else 1].astype(F32)
                for k in range(2):
                    xs[pl.ds(2 * pitch + col + k, height, stride=pitch), :] = value[:, k * c : (k + 1) * c]
            else:
                value = corners[(0 if dy > 0 else 2) + (0 if dx > 0 else 1)].astype(F32)
                base = tip - 2 if dy > 0 else 0
                for r in range(2):
                    for k in range(2):
                        xs[pl.ds((row + r) * pitch + col + k, 1), :] = value[
                            base + r : base + r + 1, k * c : (k + 1) * c
                        ]

        def empty(row=row):
            for k in range(2):
                xs[pl.ds((row + k) * pitch + LEAD, breadth), :] = jnp.zeros((breadth, c), F32)

        pl.when(back)(landed)
        if dx == 0:
            pl.when(jnp.logical_not(back))(empty)

    def encode(k, carry):
        e = lax.rem(k + EARLY_AT + EARLY, steps)
        base = [p * reach + e * rows for p in range(bands)]

        @pl.when((k == 0) | (e == 0))
        def _():
            for start in base:
                fill(start, 4)
            conv_one(base, 2)

        @pl.when((lat == 0) & (e == 0))
        def _():
            fn[0:1] = nothing
            ff[0:1] = nothing

        for start in base:
            fill(start + 4, rows)
        conv_one([start + 2 for start in base], rows)

        @pl.when((lat == nlat - 1) & (e == steps - 1))
        def _():
            fn[height + 1 :] = nothing
            ff[height + 1 :] = nothing

        tail(base, e * block, UNIT)
        fresh = (e < EARLY_AT) | (e >= EARLY_AT + EARLY)
        post(e, e * block, 0, block, lambda edge: edge | fresh)
        return carry

    lax.fori_loop(0, steps, encode, 0)

    for load in loads[2 * bands + 4 :]:
        load.wait()

    def all_of(buffer, landing, send_sem, recv_sem, g):
        return pltpu.make_async_remote_copy(
            src_ref=buffer.at[pl.ds(0, count - 1)], dst_ref=landing.at[pl.ds(0, count - 1)],
            send_sem=send_sem.at[g], recv_sem=recv_sem.at[g],
            device_id=(lat, (lon + 1) % nlon), device_id_type=MESH,
        )

    per_group = steps // groups
    ahead = -(-(EARLY_AT + EARLY) // per_group)

    def attend(k, carry):
        g = lax.rem(k + ahead, groups)
        all_of(sbuf, rbuf, go_send, go_recv, g).wait_recv()
        at = pl.ds(g * count, count)
        cells_in = rbuf[at].astype(F32).reshape(count * joint * tokens, latent)
        total = window_block(joint, count, tokens, cells_in, g_ref, ai_ref, ao_ref, di_ref, do_ref)
        s2buf[at] = total.reshape(count, joint * tokens, latent).astype(BF16)

        def send(k, carry):
            peer = lax.rem(me + k, count)
            pltpu.make_async_remote_copy(
                src_ref=s2buf.at[pl.ds(g * count + peer, 1)], dst_ref=r2buf.at[pl.ds(g * count + me, 1)],
                send_sem=back_send.at[g], recv_sem=back_recv.at[g],
                device_id=peer, device_id_type=FLAT,
            ).start()
            return carry

        lax.fori_loop(1, count, send, 0)
        own = pl.ds(g * count + me, 1)
        r2buf[own] = s2buf[own]
        return carry

    lax.fori_loop(0, groups, attend, 0)

    def expand(i, carry):
        g = lax.rem(i + ahead, groups)
        all_of(s2buf, r2buf, back_send, back_recv, g).wait_recv()
        for k in range(per_group):
            e = g * per_group + k
            placed = []
            for u in range(UNIT):
                got = r2buf[pl.ds(e * block + u * span, span)].astype(F32).reshape(cells, latent)
                placed.append(dot(inward, got.astype(BF16)).astype(BF16))
            made = dot(jnp.concatenate(placed, axis=0), ew_ref[...])
            for u in range(UNIT):
                for p in range(bands):
                    top = u * cells + p * half
                    for d in range(4):
                        line = (p * rows + 2 * u + d // 2) * breadth + d % 2
                        os[pl.ds(line, half, stride=2), :] = made[top : top + half, d * c : (d + 1) * c]
            for p in range(bands):
                place = pl.ds(p * reach + e * rows, rows)
                lines = os[p * rows * breadth : (p + 1) * rows * breadth, :].reshape(rows, breadth, c)
                ost[place] = (lines + xv[place].astype(F32)).astype(BF16)
        return carry

    lax.fori_loop(0, groups, expand, 0)

    def settle(g, carry):
        all_of(sbuf, rbuf, go_send, go_recv, g).wait_send()
        all_of(s2buf, r2buf, back_send, back_recv, g).wait_send()
        return carry

    lax.fori_loop(0, groups, settle, 0)
    for _, _, there, _, copy in halo:
        pl.when(there)(copy.wait_send)


def flush_body(made_ref, out_ref, sems):
    share = made_ref.shape[0] // FLUSHES
    copies = [
        pltpu.make_async_copy(made_ref.at[pl.ds(i * share, share)], out_ref.at[pl.ds(i * share, share)], sems.at[i])
        for i in range(FLUSHES)
    ]
    for copy in copies:
        copy.start()
    for copy in copies:
        copy.wait()


def per_device(
    input_field,
    conv_one,
    conv_two,
    merge_weight,
    norm_gains,
    attention_in,
    attention_out,
    dense_in,
    dense_out,
    expand_weight,
):
    height, breadth, c = input_field.shape
    latent = merge_weight.shape[1]
    nlat = lax.axis_size("lat")
    nlon = lax.axis_size("lon")
    count = nlat * nlon
    bands = WINDOW // nlat
    per_lon = WINDOW // nlon
    offset_lat = height // (2 * bands)
    offset_lon = breadth // (2 * per_lon)
    tokens = bands * per_lon
    joint = max(1, 8 // tokens)
    entries = offset_lat * offset_lon // joint
    groups = entries // count
    half = breadth // 2
    pairs = -(-(half + 1) // 16) * 16
    pitch = -(-(LEAD + 2 * pairs) // 8) * 8
    rows = 2 * UNIT
    block = UNIT * offset_lon // joint
    args = (
        input_field, conv_one, conv_two, merge_weight, norm_gains,
        attention_in, attention_out, dense_in, dense_out, expand_weight,
    )
    geo = (nlat, nlon, bands, per_lon, offset_lat, offset_lon, pairs, joint, groups)
    message = (entries, joint * tokens, latent)
    scratch = [pltpu.VMEM(a.shape, a.dtype) for a in args]
    scratch += [
        pltpu.VMEM((12 * c, 2 * c), BF16),
        pltpu.VMEM((12 * c, 2 * c), BF16),
        pltpu.VMEM(((height + 5) * pitch, c), F32),
        pltpu.VMEM((height + 4, pairs, 2 * c), BF16),
        pltpu.VMEM((height + 4, pairs, 2 * c), BF16),
        pltpu.VMEM((bands * (rows + 2), pairs, 2 * c), F32),
        pltpu.VMEM((height + 2, half, 2 * c), BF16),
        pltpu.VMEM((height + 2, half, 2 * c), BF16),
        pltpu.VMEM((2, height, 2 * c), BF16),
        pltpu.VMEM((2, height, 2 * c), BF16),
        pltpu.VMEM((2, 2, breadth, c), BF16),
        pltpu.VMEM((4, 16, 2 * c), BF16),
        pltpu.VMEM((entries + EARLY * block,) + message[1:], BF16),
        pltpu.VMEM(message, BF16),
        pltpu.VMEM(message, BF16),
        pltpu.VMEM(message, BF16),
        pltpu.VMEM((bands * rows * breadth + 8, c), F32),
        pltpu.SemaphoreType.DMA((2 * bands + 10,)),
        pltpu.SemaphoreType.DMA((8,)),
        pltpu.SemaphoreType.DMA((8,)),
        pltpu.SemaphoreType.DMA((groups,)),
        pltpu.SemaphoreType.DMA((groups,)),
        pltpu.SemaphoreType.DMA((groups,)),
        pltpu.SemaphoreType.DMA((groups,)),
    ]
    made = pl.pallas_call(
        functools.partial(whole_body, geo),
        in_specs=[pl.BlockSpec(memory_space=pl.ANY)] * len(args),
        out_specs=pl.BlockSpec(memory_space=pltpu.VMEM),
        out_shape=pltpu.VMEM(input_field.shape, BF16),
        scratch_shapes=scratch,
        compiler_params=pltpu.CompilerParams(
            collective_id=0, has_side_effects=True, vmem_limit_bytes=LIMIT
        ),
        cost_estimate=pl.CostEstimate(flops=40_000_000_000, bytes_accessed=16_000_000, transcendentals=0),
        name="whole",
    )(*args)
    return pl.pallas_call(
        flush_body,
        in_specs=[pl.BlockSpec(memory_space=pltpu.VMEM)],
        out_specs=pl.BlockSpec(memory_space=pl.ANY),
        out_shape=jax.ShapeDtypeStruct(input_field.shape, BF16),
        scratch_shapes=[pltpu.SemaphoreType.DMA((FLUSHES,))],
        cost_estimate=pl.CostEstimate(flops=1_000_000, bytes_accessed=4_000_000, transcendentals=0),
        compiler_params=pltpu.CompilerParams(vmem_limit_bytes=4 * 1024 * 1024),
        name="flush",
    )(made)


def solution(mesh):
    return jax.shard_map(
        per_device,
        mesh=mesh,
        in_specs=(P("lat", "lon", None), P(), P(), P(), P(), P(), P(), P(), P(), P()),
        out_specs=P("lat", "lon", None),
        check_vma=False,
    )
```

```python
import functools
import math

import jax
import jax.numpy as jnp
from jax import lax
from jax.experimental import pallas as pl
from jax.experimental.pallas import tpu as pltpu
from jax.sharding import PartitionSpec as P

WINDOW = 16
HEAD_WIDTH = 32
EPSILON = 1e-06
FLOOR = 0.75
F32 = jnp.float32
BF16 = jnp.bfloat16
LIMIT = 56 * 1024 * 1024
MESH = pl.DeviceIdType.MESH
FLAT = pl.DeviceIdType.LOGICAL
LEAD = 8
UNIT = 2
FLUSHES = 8
EARLY = 2
EARLY_AT = 1


def dot(a, b):
    return jnp.dot(a, b, preferred_element_type=F32)


def ones_where(flag):
    return flag.astype(F32).astype(BF16)


def pair_kernel(kernel_ref, paired):
    taps, _, c, o = kernel_ref.shape
    zero = jnp.zeros((c, o), BF16)
    for a in range(taps):
        for b in range(4):
            rows = slice((4 * a + b) * c, (4 * a + b + 1) * c)
            paired[rows, :o] = kernel_ref[a, b] if b < 3 else zero
            paired[rows, o:] = kernel_ref[a, b - 1] if b > 0 else zero


def layer_norm(stream, gain):
    center = stream - jnp.mean(stream, axis=-1, keepdims=True)
    spread = jnp.mean(center * center, axis=-1, keepdims=True)
    return center * lax.rsqrt(spread + EPSILON) * gain


def window_block(windows, sources, tokens, cells, g_ref, ai_ref, ao_ref, di_ref, do_ref):
    latent = cells.shape[-1]
    size = sources * tokens
    count = windows * size
    coarse = cells
    if windows > 1:
        to = lax.broadcasted_iota(jnp.int32, (count, count), 0)
        of = lax.broadcasted_iota(jnp.int32, (count, count), 1)
        row = lax.broadcasted_iota(jnp.int32, (count, 1), 0)
        col = lax.broadcasted_iota(jnp.int32, (1, count), 1)

        def sorted_row(i):
            return (i // tokens % windows) * size + i // (tokens * windows) * tokens + i % tokens

        gather = ones_where(to == sorted_row(col))
        scatter = ones_where(of == sorted_row(row))
        coarse = dot(gather, cells.astype(BF16))
    gains = g_ref[...]
    normed = layer_norm(coarse, gains[0:1]).astype(BF16)
    head_row = lax.broadcasted_iota(jnp.int32, (latent, latent), 0) // HEAD_WIDTH
    head_col = lax.broadcasted_iota(jnp.int32, (latent, latent), 1) // HEAD_WIDTH
    spread = jnp.where(head_row == head_col, 1.0 / HEAD_WIDTH, 0.0).astype(BF16)

    def head_norm(stream, gain):
        square = dot((stream * stream).astype(BF16), spread)
        return (stream * gain * lax.rsqrt(jnp.maximum(square, FLOOR))).astype(BF16)

    queries = head_norm(dot(normed, ai_ref[:, :latent]), gains[1:2])
    key_rows = head_norm(dot(normed, ai_ref[:, latent : 2 * latent]), gains[2:3])
    values = dot(normed, ai_ref[:, 2 * latent :]).astype(BF16)
    group = 128
    heads = group // HEAD_WIDTH
    lane = lax.broadcasted_iota(jnp.int32, (size, group), 1) // HEAD_WIDTH
    marks = [ones_where(lane == h) for h in range(heads)]
    scale = HEAD_WIDTH ** (-0.5) * math.log2(math.e)
    parts = []
    for win in range(windows):
        span = slice(win * size, (win + 1) * size)
        row_parts = []
        for at in range(0, latent, group):
            q = queries[span, at : at + group]
            k = key_rows[span, at : at + group]
            v = values[span, at : at + group]
            expons = []
            stacked = []
            for h in range(heads):
                scores = lax.dot_general(
                    q * marks[h], k, (((1,), (1,)), ((), ())), preferred_element_type=F32
                )
                expons.append(jnp.exp2(scores * scale).astype(BF16))
                stacked.append(jnp.concatenate([v * marks[h], marks[h]], axis=1))
            both = dot(jnp.concatenate(expons, axis=1), jnp.concatenate(stacked, axis=0))
            row_parts.append((both[:, :group] / both[:, group:]).astype(BF16))
        parts.append(jnp.concatenate(row_parts, axis=1))
    attended = jnp.concatenate(parts, axis=0)
    mixed = (coarse + dot(attended, ao_ref[...])).astype(BF16)
    normed_two = layer_norm(mixed.astype(F32), gains[3:4]).astype(BF16)
    total = mixed.astype(F32)
    width = di_ref.shape[1]
    step = min(512, width)
    for at in range(0, width, step):
        inner = jax.nn.gelu(dot(normed_two, di_ref[:, at : at + step])).astype(BF16)
        total = total + dot(inner, do_ref[at : at + step, :])
    if windows > 1:
        total = dot(scatter, total.astype(BF16))
    return total


def whole_body(geo, x_hbm, k1_hbm, k2_hbm, mw_hbm, g_hbm, ai_hbm, ao_hbm, di_hbm, do_hbm, ew_hbm, ost,
               xv, k1_ref, k2_ref, mw_ref, g_ref, ai_ref, ao_ref, di_ref, do_ref, ew_ref,
               w1_ref, w2_ref, xs, xn, xf, fs, fn, ff, edges, sides, caps, corners,
               sbuf, rbuf, s2buf, r2buf, os,
               load_sem, halo_send, halo_recv, go_send, go_recv, back_send, back_recv):
    (nlat, nlon, bands, per_lon, offset_lat, offset_lon, pairs, joint, groups) = geo
    count = nlat * nlon
    lat = lax.axis_index("lat")
    lon = lax.axis_index("lon")
    me = lat * nlon + lon
    height, breadth, c = xv.shape
    half = breadth // 2
    latent = 4 * c
    tokens = bands * per_lon
    cells = bands * half
    reach = 2 * offset_lat
    rows = 2 * UNIT
    steps = offset_lat // UNIT
    block = UNIT * offset_lon // joint
    pitch = xs.shape[0] // (height + 5)

    head = EARLY_AT * rows - 2
    depth = rows + 4
    firsts = [pl.ds(p * reach + head, depth) for p in range(bands)]
    stops = [0] + [p * reach + head + depth for p in range(bands)]
    rests = [
        pl.ds(stop, (p * reach + head if p < bands else height) - stop) for p, stop in enumerate(stops)
    ]
    pieces = [(x_hbm.at[at], xv.at[at]) for at in firsts]
    pieces += [(k1_hbm, k1_ref), (k2_hbm, k2_ref), (mw_hbm, mw_ref)]
    pieces += [(x_hbm.at[at], xv.at[at]) for at in rests]
    pieces += [(g_hbm, g_ref), (ai_hbm, ai_ref), (ao_hbm, ao_ref), (di_hbm, di_ref), (do_hbm, do_ref), (ew_hbm, ew_ref)]
    loads = [pltpu.make_async_copy(a, b, load_sem.at[i]) for i, (a, b) in enumerate(pieces)]
    for load in loads[: bands + 3]:
        load.start()

    barrier = pltpu.get_barrier_semaphore()

    def greet(k, carry):
        pl.semaphore_signal(barrier, inc=1, device_id=lax.rem(me + k, count), device_id_type=FLAT)
        return carry

    lax.fori_loop(1, count, greet, 0)
    for load in loads[bands + 3 :]:
        load.start()

    def widen(r, carry):
        for k in range(4):
            at = 4 * r + k
            xs[pl.ds((at + 2) * pitch + LEAD, breadth), :] = xv[at].astype(F32)
        return carry

    def column(at):
        return xs[pl.ds(2 * pitch + LEAD + at, height, stride=pitch), :]

    left, right = LEAD - 2, LEAD + breadth
    for col in (left, left + 1, right, right + 1):
        xs[pl.ds(col, height + 4, stride=pitch), :] = jnp.zeros((height + 4, c), F32)

    for p in range(bands):
        loads[p].wait()
        for r in range(depth):
            at = p * reach + head + r
            xs[pl.ds((at + 2) * pitch + LEAD, breadth), :] = xv[at].astype(F32)
    loads[bands].wait()
    pair_kernel(k1_ref, w1_ref)

    def fill(start, n):
        for r in range(n):
            base = (start + r) * pitch + left
            quad = [xs[pl.ds(base + j, pairs, stride=2), :] for j in range(4)]
            xn[pl.ds(start + r, 1)] = jnp.concatenate(quad[:2], axis=1).astype(BF16)[None]
            xf[pl.ds(start + r, 1)] = jnp.concatenate(quad[2:], axis=1).astype(BF16)[None]

    pair = lax.broadcasted_iota(jnp.int32, (pairs, 2 * c), 0)
    lane = lax.broadcasted_iota(jnp.int32, (pairs, 2 * c), 1)
    lon_place = 2 * pair + (lane >= c).astype(jnp.int32) + (lon * breadth - 1)
    inside = (lon_place >= 0) & (lon_place < nlon * breadth)

    def conv_one(starts, n):
        lhs = jnp.concatenate(
            [
                jnp.concatenate(
                    [buf[pl.ds(start + a, n)].reshape(n * pairs, 2 * c) for start in starts], axis=0
                )
                for a in range(3)
                for buf in (xn, xf)
            ],
            axis=1,
        )
        first = jax.nn.gelu(dot(lhs, w1_ref[...])).reshape(bands * n, pairs, 2 * c)
        fs[: bands * n] = jnp.where(inside[None], first, 0.0)
        for p, start in enumerate(starts):
            fn[pl.ds(start, n)] = fs[p * n : (p + 1) * n, 0:half, :].astype(BF16)
            ff[pl.ds(start, n)] = fs[p * n : (p + 1) * n, pl.ds(1, half), :].astype(BF16)

    to = lax.broadcasted_iota(jnp.int32, (cells, cells), 0)
    of = lax.broadcasted_iota(jnp.int32, (cells, cells), 1)
    outward = ones_where(of == (to % tokens) * offset_lon + to // tokens)
    inward = ones_where(of == (to % offset_lon) * tokens + to // offset_lon)

    span = offset_lon // joint
    nothing = jnp.zeros((1, half, 2 * c), BF16)

    def tail(base, place, units):
        lines = 2 * units
        lhs = jnp.concatenate(
            [
                jnp.concatenate(
                    [buf[pl.ds(start + a, lines)].reshape(lines * half, 2 * c) for start in base], axis=0
                )
                for a in range(3)
                for buf in (fn, ff)
            ],
            axis=1,
        )
        second = jax.nn.gelu(dot(lhs, w2_ref[...])).astype(BF16)
        second = second.reshape(bands * units, 2, half, 2 * c)
        patches = jnp.concatenate(
            [second[:, d].reshape(bands * units * half, 2 * c) for d in range(2)], axis=1
        )
        coarse = dot(patches, mw_ref[...]).astype(BF16).reshape(bands, units, half, latent)
        for u in range(units):
            moved = dot(outward, coarse[:, u].reshape(cells, latent))
            sbuf[pl.ds(place + u * span, span)] = moved.reshape(span, joint * tokens, latent).astype(BF16)


    def post(e, place, low, n, chosen):
        def send(k, carry):
            i = low + lax.rem(me + k, n)
            entry = e * block + i
            peer = i if block == count else lax.rem(entry, count)
            group = e if block == count else lax.div(entry, count)
            spot = lax.rem(i, span)
            take = chosen((spot == 0) | (spot == span - 1))

            @pl.when(take & (peer != me))
            def _():
                pltpu.make_async_remote_copy(
                    src_ref=sbuf.at[pl.ds(place + i, 1)], dst_ref=rbuf.at[pl.ds(group * count + me, 1)],
                    send_sem=go_send.at[group], recv_sem=go_recv.at[group],
                    device_id=peer, device_id_type=FLAT,
                ).start()

            @pl.when(take & (peer == me))
            def _():
                rbuf[pl.ds(entry, 1)] = sbuf[pl.ds(place + i, 1)]

            return carry

        lax.fori_loop(1, n + 1, send, 0)

    def early(j, low, units):
        e = EARLY_AT + j
        base = [p * reach + e * rows + 2 * low for p in range(bands)]
        fresh = j == 0 and low == 0
        more = 2 if fresh else 0
        for start in base:
            fill(start + 4 - 2 * more, 2 * units + 2 * more)
        conv_one([start + 2 - more for start in base], 2 * units + more)
        if fresh:
            loads[bands + 1].wait()
            pair_kernel(k2_ref, w2_ref)
            loads[bands + 2].wait()
        tail(base, (steps + j) * block + low * span, units)

    def early_post(j, low, units):
        post(EARLY_AT + j, (steps + j) * block, low * span, units * span, jnp.logical_not)

    early(0, 0, 1)
    pl.semaphore_wait(barrier, count - 1)
    early_post(0, 0, 1)
    for low in range(1, UNIT):
        early(0, low, 1)
        early_post(0, low, 1)

    for load in loads[bands + 3 : 2 * bands + 4]:
        load.wait()
    lax.fori_loop(0, height // 4, widen, 0)
    for side, at in enumerate((0, breadth - 2)):
        edges[side] = jnp.concatenate([column(at), column(at + 1)], axis=1).astype(BF16)

    tip = 16
    ends = (slice(0, tip), slice(height - tip, height))
    halo = []
    for i, (dy, dx) in enumerate(((-1, 0), (1, 0), (0, -1), (0, 1), (-1, -1), (-1, 1), (1, -1), (1, 1))):
        if dx == 0:
            src = xv.at[pl.ds(0 if dy < 0 else height - 2, 2)]
            dst = caps.at[1 if dy < 0 else 0]
        elif dy == 0:
            src = edges.at[0 if dx < 0 else 1]
            dst = sides.at[1 if dx < 0 else 0]
        else:
            first = 0 if dy < 0 else height - tip
            src = edges.at[0 if dx < 0 else 1, pl.ds(first, tip)]
            dst = corners.at[(2 if dy < 0 else 0) + (1 if dx < 0 else 0)]
        there = (lat + dy >= 0) & (lat + dy < nlat) & (lon + dx >= 0) & (lon + dx < nlon)
        back = (lat - dy >= 0) & (lat - dy < nlat) & (lon - dx >= 0) & (lon - dx < nlon)
        copy = pltpu.make_async_remote_copy(
            src_ref=src, dst_ref=dst, send_sem=halo_send.at[i], recv_sem=halo_recv.at[i],
            device_id=(jnp.clip(lat + dy, 0, nlat - 1), jnp.clip(lon + dx, 0, nlon - 1)), device_id_type=MESH,
        )
        halo.append((dy, dx, there, back, copy))
        pl.when(there)(copy.start)

    for j in range(1, EARLY):
        early(j, 0, UNIT)
        early_post(j, 0, UNIT)

    for dy, dx, there, back, copy in halo:
        row = 0 if dy > 0 else height + 2
        col = left if dx > 0 else right

        def landed(dy=dy, dx=dx, copy=copy, row=row, col=col):
            copy.wait_recv()
            if dx == 0:
                for k in range(2):
                    xs[pl.ds((row + k) * pitch + LEAD, breadth), :] = caps[0 if dy > 0 else 1, k].astype(F32)
            elif dy == 0:
                value = sides[0 if dx > 0 else 1].astype(F32)
                for k in range(2):
                    xs[pl.ds(2 * pitch + col + k, height, stride=pitch), :] = value[:, k * c : (k + 1) * c]
            else:
                value = corners[(0 if dy > 0 else 2) + (0 if dx > 0 else 1)].astype(F32)
                base = tip - 2 if dy > 0 else 0
                for r in range(2):
                    for k in range(2):
                        xs[pl.ds((row + r) * pitch + col + k, 1), :] = value[
                            base + r : base + r + 1, k * c : (k + 1) * c
                        ]

        def empty(row=row):
            for k in range(2):
                xs[pl.ds((row + k) * pitch + LEAD, breadth), :] = jnp.zeros((breadth, c), F32)

        pl.when(back)(landed)
        if dx == 0:
            pl.when(jnp.logical_not(back))(empty)

    def encode(k, carry):
        e = lax.rem(k + EARLY_AT + EARLY, steps)
        base = [p * reach + e * rows for p in range(bands)]

        @pl.when((k == 0) | (e == 0))
        def _():
            for start in base:
                fill(start, 4)
            conv_one(base, 2)

        @pl.when((lat == 0) & (e == 0))
        def _():
            fn[0:1] = nothing
            ff[0:1] = nothing

        for start in base:
            fill(start + 4, rows)
        conv_one([start + 2 for start in base], rows)

        @pl.when((lat == nlat - 1) & (e == steps - 1))
        def _():
            fn[height + 1 :] = nothing
            ff[height + 1 :] = nothing

        tail(base, e * block, UNIT)
        fresh = (e < EARLY_AT) | (e >= EARLY_AT + EARLY)
        post(e, e * block, 0, block, lambda edge: edge | fresh)
        return carry

    lax.fori_loop(0, steps, encode, 0)

    for load in loads[2 * bands + 4 :]:
        load.wait()

    def all_of(buffer, landing, send_sem, recv_sem, g):
        return pltpu.make_async_remote_copy(
            src_ref=buffer.at[pl.ds(0, count - 1)], dst_ref=landing.at[pl.ds(0, count - 1)],
            send_sem=send_sem.at[g], recv_sem=recv_sem.at[g],
            device_id=(lat, (lon + 1) % nlon), device_id_type=MESH,
        )

    per_group = steps // groups
    ahead = -(-(EARLY_AT + EARLY) // per_group)

    def attend(k, carry):
        g = lax.rem(k + ahead, groups)
        all_of(sbuf, rbuf, go_send, go_recv, g).wait_recv()
        at = pl.ds(g * count, count)
        cells_in = rbuf[at].astype(F32).reshape(count * joint * tokens, latent)
        total = window_block(joint, count, tokens, cells_in, g_ref, ai_ref, ao_ref, di_ref, do_ref)
        s2buf[at] = total.reshape(count, joint * tokens, latent).astype(BF16)

        def send(k, carry):
            peer = lax.rem(me + k, count)
            pltpu.make_async_remote_copy(
                src_ref=s2buf.at[pl.ds(g * count + peer, 1)], dst_ref=r2buf.at[pl.ds(g * count + me, 1)],
                send_sem=back_send.at[g], recv_sem=back_recv.at[g],
                device_id=peer, device_id_type=FLAT,
            ).start()
            return carry

        lax.fori_loop(1, count, send, 0)
        own = pl.ds(g * count + me, 1)
        r2buf[own] = s2buf[own]
        return carry

    lax.fori_loop(0, groups, attend, 0)

    def expand(i, carry):
        g = lax.rem(i + ahead, groups)
        all_of(s2buf, r2buf, back_send, back_recv, g).wait_recv()
        for k in range(per_group):
            e = g * per_group + k
            placed = []
            for u in range(UNIT):
                got = r2buf[pl.ds(e * block + u * span, span)].astype(F32).reshape(cells, latent)
                placed.append(dot(inward, got.astype(BF16)).astype(BF16))
            made = dot(jnp.concatenate(placed, axis=0), ew_ref[...])
            for u in range(UNIT):
                for p in range(bands):
                    top = u * cells + p * half
                    for d in range(4):
                        line = (p * rows + 2 * u + d // 2) * breadth + d % 2
                        os[pl.ds(line, half, stride=2), :] = made[top : top + half, d * c : (d + 1) * c]
            for p in range(bands):
                place = pl.ds(p * reach + e * rows, rows)
                lines = os[p * rows * breadth : (p + 1) * rows * breadth, :].reshape(rows, breadth, c)
                ost[place] = (lines + xv[place].astype(F32)).astype(BF16)
        return carry

    lax.fori_loop(0, groups, expand, 0)

    def settle(g, carry):
        all_of(sbuf, rbuf, go_send, go_recv, g).wait_send()
        all_of(s2buf, r2buf, back_send, back_recv, g).wait_send()
        return carry

    lax.fori_loop(0, groups, settle, 0)
    for _, _, there, _, copy in halo:
        pl.when(there)(copy.wait_send)


def flush_body(made_ref, out_ref, sems):
    share = made_ref.shape[0] // FLUSHES
    copies = [
        pltpu.make_async_copy(made_ref.at[pl.ds(i * share, share)], out_ref.at[pl.ds(i * share, share)], sems.at[i])
        for i in range(FLUSHES)
    ]
    for copy in copies:
        copy.start()
    for copy in copies:
        copy.wait()


def per_device(
    input_field,
    conv_one,
    conv_two,
    merge_weight,
    norm_gains,
    attention_in,
    attention_out,
    dense_in,
    dense_out,
    expand_weight,
):
    height, breadth, c = input_field.shape
    latent = merge_weight.shape[1]
    nlat = lax.axis_size("lat")
    nlon = lax.axis_size("lon")
    count = nlat * nlon
    bands = WINDOW // nlat
    per_lon = WINDOW // nlon
    offset_lat = height // (2 * bands)
    offset_lon = breadth // (2 * per_lon)
    tokens = bands * per_lon
    joint = max(1, 8 // tokens)
    entries = offset_lat * offset_lon // joint
    groups = entries // count
    half = breadth // 2
    pairs = -(-(half + 1) // 16) * 16
    pitch = -(-(LEAD + 2 * pairs) // 8) * 8
    rows = 2 * UNIT
    block = UNIT * offset_lon // joint
    args = (
        input_field, conv_one, conv_two, merge_weight, norm_gains,
        attention_in, attention_out, dense_in, dense_out, expand_weight,
    )
    geo = (nlat, nlon, bands, per_lon, offset_lat, offset_lon, pairs, joint, groups)
    message = (entries, joint * tokens, latent)
    scratch = [pltpu.VMEM(a.shape, a.dtype) for a in args]
    scratch += [
        pltpu.VMEM((12 * c, 2 * c), BF16),
        pltpu.VMEM((12 * c, 2 * c), BF16),
        pltpu.VMEM(((height + 5) * pitch, c), F32),
        pltpu.VMEM((height + 4, pairs, 2 * c), BF16),
        pltpu.VMEM((height + 4, pairs, 2 * c), BF16),
        pltpu.VMEM((bands * (rows + 2), pairs, 2 * c), F32),
        pltpu.VMEM((height + 2, half, 2 * c), BF16),
        pltpu.VMEM((height + 2, half, 2 * c), BF16),
        pltpu.VMEM((2, height, 2 * c), BF16),
        pltpu.VMEM((2, height, 2 * c), BF16),
        pltpu.VMEM((2, 2, breadth, c), BF16),
        pltpu.VMEM((4, 16, 2 * c), BF16),
        pltpu.VMEM((entries + EARLY * block,) + message[1:], BF16),
        pltpu.VMEM(message, BF16),
        pltpu.VMEM(message, BF16),
        pltpu.VMEM(message, BF16),
        pltpu.VMEM((bands * rows * breadth + 8, c), F32),
        pltpu.SemaphoreType.DMA((2 * bands + 10,)),
        pltpu.SemaphoreType.DMA((8,)),
        pltpu.SemaphoreType.DMA((8,)),
        pltpu.SemaphoreType.DMA((groups,)),
        pltpu.SemaphoreType.DMA((groups,)),
        pltpu.SemaphoreType.DMA((groups,)),
        pltpu.SemaphoreType.DMA((groups,)),
    ]
    made = pl.pallas_call(
        functools.partial(whole_body, geo),
        in_specs=[pl.BlockSpec(memory_space=pl.ANY)] * len(args),
        out_specs=pl.BlockSpec(memory_space=pltpu.VMEM),
        out_shape=pltpu.VMEM(input_field.shape, BF16),
        scratch_shapes=scratch,
        compiler_params=pltpu.CompilerParams(
            collective_id=0, has_side_effects=True, vmem_limit_bytes=LIMIT
        ),
        cost_estimate=pl.CostEstimate(flops=40_000_000_000, bytes_accessed=16_000_000, transcendentals=0),
        name="whole",
    )(*args)
    return pl.pallas_call(
        flush_body,
        in_specs=[pl.BlockSpec(memory_space=pltpu.VMEM)],
        out_specs=pl.BlockSpec(memory_space=pl.ANY),
        out_shape=jax.ShapeDtypeStruct(input_field.shape, BF16),
        scratch_shapes=[pltpu.SemaphoreType.DMA((FLUSHES,))],
        cost_estimate=pl.CostEstimate(flops=1_000_000, bytes_accessed=4_000_000, transcendentals=0),
        compiler_params=pltpu.CompilerParams(vmem_limit_bytes=4 * 1024 * 1024),
        name="flush",
    )(made)


def solution(mesh):
    return jax.shard_map(
        per_device,
        mesh=mesh,
        in_specs=(P("lat", "lon", None), P(), P(), P(), P(), P(), P(), P(), P(), P()),
        out_specs=P("lat", "lon", None),
        check_vma=False,
    )
```
